32 devices in a mesh: ta: 16 (over z, y, x), sa: 2 (over core).
Axes of the slice: x: 2, y: 2, z: 4, core: 2. Of those that a mesh axis runs over, the one named last changes fastest.
Arguments:
- rhs: float32 [1, 2, 40, 16, 2, 128], P(None, None, None, 'ta', 'sa'), may hold values from -6 to 6
- links: bfloat16 [4, 2, 40, 40, 16, 2, 128], P(None, None, None, None, 'ta', 'sa'), may hold values from -0.625 to 0.625
- clover: bfloat16 [2, 40, 40, 16, 2, 128], P(None, None, None, 'ta', 'sa'), may hold values from -1 to 7
- mr_steps: int32 [16, 2, 2], P('ta', 'sa'), may hold values from 2 to 3
Outputs:
- solution: float32 [1, 2, 40, 16, 2, 128], P(None, None, None, 'ta', 'sa')
- residual: float32 [1, 2, 40, 16, 2, 128], P(None, None, None, 'ta', 'sa')
The draws below stay inside these ranges and needn't reach their ends.
All inputs are finite; a program needn't handle non-finite values.
Results may differ from the reference program's by a relative error of at most 0.0003.
Values sent between devices are 32-bit elements; how exact they have to be, the bound alone decides.
No kernel may reach another device: no remote copies, remote signals or barrier semaphores. Data moves between devices by JAX's collectives and lax.ppermute only.
A program may use at most 128 MiB of HBM per device.

```python
import jax
import jax.numpy as jnp
from jax import lax

NVEC = 20
DOF = 40
NRHS = 1
TD = 2
LZ = 4
LY = 4
LX = 4
MR_MAX = 3
SWEEPS = 2
NTD = 16
NZD = 2
DS = 128


def draw_clover(key, part):
    folded = jax.random.fold_in(key, 7)
    first, second = jax.random.split(folded)
    shape = (2, DOF, DOF, NTD, NZD, DS)
    spread = jax.random.normal(first, shape, jnp.float32) / jnp.sqrt(jnp.float32(DOF))
    diagonal = jax.random.uniform(second, (NTD, NZD, DS), jnp.float32, 3.5, 5.0)
    spread = jnp.clip(spread, -1.0, 1.0)
    identity = jnp.eye(DOF, dtype=jnp.float32)[:, :, None, None, None]
    real_part = spread[0] + identity * diagonal[None, None]
    return jnp.stack([real_part, spread[1]], 0).astype(jnp.bfloat16)


def with_ends(array, rng, low, largest):
    spot = [jax.random.randint(jax.random.fold_in(rng, axis), (), 0, length) for axis, length in enumerate(array.shape)]
    longest = array.shape.index(max(array.shape))
    neighbour = spot[:longest] + [(spot[longest] + 1) % array.shape[longest]] + spot[longest + 1:]
    return array.at[tuple(spot)].set(low).at[tuple(neighbour)].set(largest)


def levels(own_key, shape, cuts, smallest, top_value):
    factor_of = 1.0
    for axis_at, shards_of in cuts:
        draws = jax.random.uniform(jax.random.fold_in(jax.random.fold_in(own_key, 6), axis_at), (shards_of,), jnp.float32, smallest / len(cuts), top_value / len(cuts))
        factor_of = factor_of * jnp.repeat(jnp.exp(draws), shape[axis_at] // shards_of).reshape((-1,) + (1,) * (len(shape) - 1 - axis_at))
    return factor_of


def bell_draw(own_key, shape, deviation, most, cuts=(), kind=jnp.bfloat16):
    values = deviation * jax.random.normal(own_key, shape, jnp.float32)
    if cuts:
        values = values * levels(own_key, shape, cuts, -0.22, 0.18)
    return jnp.clip(values, -most, most).astype(kind)


def setup_inputs(seed: int = 0) -> dict:
    key_list = jax.random.split(jax.random.key(seed), 5)
    rhs = bell_draw(key_list[0], (NRHS, 2, DOF, NTD, NZD, DS), 1.0, 6.0, ((3, 16), (4, 2)), jnp.float32)
    links = bell_draw(key_list[1], (4, 2, DOF, DOF, NTD, NZD, DS), (2 * DOF) ** -0.5, 0.625, ((4, 16), (5, 2)))
    clover = draw_clover(jax.random.fold_in(key_list[4], 71), 0)
    mr_steps = with_ends(jax.random.randint(key_list[3], (NTD, NZD, 2), 2, MR_MAX + 1), jax.random.fold_in(key_list[3], 1), 2, MR_MAX).astype(jnp.int32)
    return {"rhs": rhs, "links": links, "clover": clover, "mr_steps": mr_steps}


HIGHEST = lax.Precision.HIGHEST


def complex_apply(matrices, vectors, dagger):
    real_mat = matrices[0].astype(jnp.float32)
    imag_mat = matrices[1].astype(jnp.float32)
    real_vec = vectors[:, 0]
    imag_vec = vectors[:, 1]
    pattern = "ji...,rj...->ri..." if dagger else "ij...,rj...->ri..."

    def product(left, right):
        return jnp.einsum(pattern, left, right, precision=HIGHEST)

    if dagger:
        real_out = product(real_mat, real_vec) + product(imag_mat, imag_vec)
        imag_out = product(real_mat, imag_vec) - product(imag_mat, real_vec)
    else:
        real_out = product(real_mat, real_vec) - product(imag_mat, imag_vec)
        imag_out = product(real_mat, imag_vec) + product(imag_mat, real_vec)
    return jnp.stack([real_out, imag_out], axis=1)


def lattice_view(field):
    leading = field.shape[:3]
    shaped = field.reshape(leading + (NTD, NZD, TD, LZ, LY, LX))
    shaped = jnp.transpose(shaped, (0, 1, 2, 3, 5, 4, 6, 7, 8))
    return shaped.reshape(leading + (NTD * TD, NZD * LZ, LY, LX))


def domain_view(lattice):
    leading = lattice.shape[:3]
    shaped = lattice.reshape(leading + (NTD, TD, NZD, LZ, LY, LX))
    shaped = jnp.transpose(shaped, (0, 1, 2, 3, 5, 4, 6, 7, 8))
    return shaped.reshape(leading + (NTD, NZD, DS))


def shifted(field, direction, amount):
    return domain_view(jnp.roll(lattice_view(field), amount, axis=3 + direction))


def apply_operator(field, links, clover):
    signs = jnp.where(jnp.arange(DOF) < NVEC, 1.0, -1.0).astype(jnp.float32)[:, None, None]

    def backward_terms(index):
        vectors = lax.dynamic_index_in_dim(field, index, 3, keepdims=False)
        matrices = lax.dynamic_index_in_dim(links, index, 4, keepdims=False)
        return jnp.stack([signs * complex_apply(matrices[direction], signs * vectors, True) for direction in range(4)], 0)

    back_terms = jnp.moveaxis(lax.map(backward_terms, jnp.arange(NTD)), 0, 4)
    neighbours = jnp.stack([shifted(field, direction, -1) for direction in range(4)], 0)
    behind_total = shifted(back_terms[0], 0, 1)
    for direction in range(1, 4):
        behind_total = behind_total + shifted(back_terms[direction], direction, 1)

    def forward_terms(index):
        vectors = lax.dynamic_index_in_dim(field, index, 3, keepdims=False)
        nearby = lax.dynamic_index_in_dim(neighbours, index, 4, keepdims=False)
        matrices = lax.dynamic_index_in_dim(links, index, 4, keepdims=False)
        self_block = lax.dynamic_index_in_dim(clover, index, 3, keepdims=False)
        total = complex_apply(self_block, vectors, False)
        for direction in range(4):
            total = total - complex_apply(matrices[direction], nearby[direction], False)
        return total

    result = jnp.moveaxis(lax.map(forward_terms, jnp.arange(NTD)), 0, 3)
    return result - behind_total


def block_sums(component):
    shaped = component.reshape(component.shape[:4] + (2, DS // 2))
    return jnp.sum(shaped, axis=(1, 5))


def block_scale(factor, component):
    shaped = component.reshape(component.shape[:4] + (2, DS // 2))
    return (factor[:, None, :, :, :, None] * shaped).reshape(component.shape)


def reference(rhs, links, clover, mr_steps):
    colour = (jnp.arange(DS)[None, :] // (DS // 2) + jnp.arange(NZD)[:, None]) % 2
    solution = jnp.zeros_like(rhs)
    for sweep_index in range(SWEEPS):
        for colour_index in range(2):
            mask = (colour == colour_index).astype(jnp.float32)
            remainder = rhs - apply_operator(solution, links, clover)
            search = remainder * mask
            correction = jnp.zeros_like(search)
            for step_index in range(MR_MAX):
                image = apply_operator(search, links, clover) * mask
                real_s = search[:, 0]
                imag_s = search[:, 1]
                real_q = image[:, 0]
                imag_q = image[:, 1]
                numer_real = block_sums(real_q * real_s + imag_q * imag_s)
                numer_imag = block_sums(real_q * imag_s - imag_q * real_s)
                denom = block_sums(real_q * real_q + imag_q * imag_q) + 1e-6
                live = (step_index < mr_steps)[None]
                alpha_real = jnp.where(live, numer_real / denom, 0.0)
                alpha_imag = jnp.where(live, numer_imag / denom, 0.0)
                correction = correction + jnp.stack([block_scale(alpha_real, real_s) - block_scale(alpha_imag, imag_s), block_scale(alpha_real, imag_s) + block_scale(alpha_imag, real_s)], 1)
                search = search - jnp.stack([block_scale(alpha_real, real_q) - block_scale(alpha_imag, imag_q), block_scale(alpha_real, imag_q) + block_scale(alpha_imag, real_q)], 1)
            solution = solution + correction
    residual = rhs - apply_operator(solution, links, clover)
    return solution, residual
```

```python
import functools

import jax
import jax.numpy as jnp
from jax import lax
from jax.experimental import pallas as pl
from jax.experimental.pallas import tpu as pltpu
from jax.sharding import PartitionSpec as P

LZ = 4
LY = 4
LX = 4
MR_MAX = 3
SWEEPS = 2
PLANE = LY * LX

F32 = jnp.float32
VMEM = pl.BlockSpec(memory_space=pltpu.VMEM)
SMEM = pl.BlockSpec(memory_space=pltpu.SMEM)
ANY = pl.BlockSpec(memory_space=pl.ANY)


def lanes(shape):
    return lax.broadcasted_iota(jnp.int32, shape, len(shape) - 1)


def low_half(shape):
    return lanes(shape) < shape[-1] // 2


def swap(x):
    return pltpu.roll(x, x.shape[-1] // 2, x.ndim - 1)


def turn(x, amount):
    return pltpu.roll(x, amount % x.shape[-1], x.ndim - 1)


def chirality(dof, width):
    rows = lax.broadcasted_iota(jnp.int32, (dof, width), 0)
    return jnp.where(rows < dof // 2, 1.0, -1.0).astype(F32)


def ahead(x, direction):
    place = lanes(x.shape) % (x.shape[-1] // 2)
    if direction == 1:
        return jnp.where(place // PLANE == LZ - 1, 0.0, turn(x, -PLANE))
    if direction == 2:
        return jnp.where(place // LX % LY == LY - 1, turn(x, (LY - 1) * LX), turn(x, -LX))
    return jnp.where(place % LX == LX - 1, turn(x, LX - 1), turn(x, -1))


def behind(x, direction):
    place = lanes(x.shape) % (x.shape[-1] // 2)
    if direction == 1:
        return jnp.where(place // PLANE == 0, 0.0, turn(x, PLANE))
    if direction == 2:
        return jnp.where(place // LX % LY == 0, turn(x, -(LY - 1) * LX), turn(x, LX))
    return jnp.where(place % LX == 0, turn(x, -(LX - 1)), turn(x, 1))


def fold(p, q):
    low = low_half(p.shape)
    return jnp.where(low, p, q) + swap(jnp.where(low, q, p))


def gather_rows(parts):
    rows = lax.broadcasted_iota(jnp.int32, parts[0].shape, 0)
    step = 1
    while len(parts) > 1:
        upper = (rows & step) != 0
        parts = [
            jnp.where(upper, odd, even) + pltpu.roll(jnp.where(upper, even, odd), step, 0)
            for even, odd in zip(parts[0::2], parts[1::2])
        ]
        step *= 2
    return parts[0]


def tile_sum(x):
    total = x[0:8]
    for start in range(8, x.shape[0], 8):
        total = total + x[start:start + 8]
    return total


def block_terms(group, terms, back_ref):
    p = [None] * 8
    q = [None] * 8
    for term, (slab, a_get, b_get, c_ref, d_ref) in enumerate(terms):
        a = a_get() if a_get is not None else None
        b = b_get() if b_get is not None else None
        if c_ref is not None:
            back_p = back_ref[term, 0]
            back_q = back_ref[term, 1]
        for k in range(8):
            row = group * 8 + k
            m = slab(row)
            if a is not None:
                pa = tile_sum(m * a)
                qa = tile_sum(m * b)
                p[k] = pa if p[k] is None else p[k] + pa
                q[k] = qa if q[k] is None else q[k] + qa
            if c_ref is not None:
                c = jnp.broadcast_to(c_ref[pl.ds(row, 1), :], m.shape)
                d = jnp.broadcast_to(d_ref[pl.ds(row, 1), :], m.shape)
                back_p = back_p + m * c
                back_q = back_q + m * d
        if c_ref is not None:
            back_ref[term, 0] = back_p
            back_ref[term, 1] = back_q
    if p[0] is None:
        return None
    return fold(gather_rows(p), gather_rows(q))


def spread_forward(x, ab_ref, slot):
    sign = jnp.where(low_half(x.shape), 1.0, -1.0)
    ab_ref[slot, 0] = x * sign
    ab_ref[slot, 1] = swap(x)


def spread_backward(x, cd_ref):
    signs = chirality(*x.shape)
    conj = jnp.where(low_half(x.shape), 1.0, -1.0)
    cd_ref[0] = x * signs
    cd_ref[1] = swap(x) * conj * signs


def block_operator(x, m_ref, ab_ref, cd_ref, back_ref, out_ref):
    dof, width = x.shape
    spread_forward(x, ab_ref, 0)
    for direction in (1, 2, 3):
        spread_forward(-ahead(x, direction), ab_ref, direction)
    spread_backward(x, cd_ref)
    back_ref[...] = jnp.zeros_like(back_ref)

    def group_body(group, carry):
        terms = []
        for term in range(4):
            terms.append((
                lambda row, term=term: m_ref[term, row],
                lambda term=term: ab_ref[term, 0],
                lambda term=term: ab_ref[term, 1],
                cd_ref.at[0] if term else None,
                cd_ref.at[1] if term else None,
            ))
        out_ref[pl.ds(pl.multiple_of(group * 8, 8), 8), :] = block_terms(group, terms, back_ref)
        return carry

    lax.fori_loop(0, dof // 8, group_body, 0)
    signs = chirality(dof, width)
    backs = [signs * fold(back_ref[d, 0], back_ref[d, 1]) for d in (1, 2, 3)]
    total = out_ref[...]
    for direction in (1, 2, 3):
        total = total - behind(backs[direction - 1], direction)
    return total, backs[0]


def backward_product(x, slab, cd_ref, back_ref):
    dof, width = x.shape
    spread_backward(x, cd_ref)
    back_ref[0] = jnp.zeros_like(back_ref[0])

    def group_body(group, carry):
        block_terms(group, [(slab, None, None, cd_ref.at[0], cd_ref.at[1])], back_ref)
        return carry

    lax.fori_loop(0, dof // 8, group_body, 0)
    return chirality(dof, width) * fold(back_ref[0, 0], back_ref[0, 1])


def forward_product(slabs, ab_ref, out_ref, dof):
    def group_body(group, carry):
        terms = [
            (slab, lambda slot=slot: ab_ref[slot, 0], lambda slot=slot: ab_ref[slot, 1], None, None)
            for slab, slot in slabs
        ]
        out_ref[pl.ds(pl.multiple_of(group * 8, 8), 8), :] = block_terms(group, terms, None)
        return carry

    lax.fori_loop(0, dof // 8, group_body, 0)
    return out_ref[...]


def total_of(x):
    return jnp.sum(jnp.sum(x, axis=0, keepdims=True), axis=1, keepdims=True)


def times(alpha_re, alpha_im, x):
    conj = jnp.where(low_half(x.shape), -1.0, 1.0)
    return alpha_re * x + alpha_im * (swap(x) * conj)


def relax(residual, steps, m_ref, s_ref, e_ref, w_ref, ab_ref, cd_ref, back_ref, out_ref):
    s_ref[...] = residual
    e_ref[...] = jnp.zeros_like(residual)
    w_ref[...] = jnp.zeros_like(residual)
    conj = jnp.where(low_half(residual.shape), 1.0, -1.0)

    def step(_, carry):
        s = s_ref[...]
        q, back_z = block_operator(s, m_ref, ab_ref, cd_ref, back_ref, out_ref)
        s = s_ref[...]
        scale = total_of(q * q) + 1e-6
        alpha_re = total_of(q * s) / scale
        alpha_im = total_of(q * (swap(s) * conj)) / scale
        e_ref[...] += times(alpha_re, alpha_im, s)
        w_ref[...] += times(alpha_re, alpha_im, back_z)
        s_ref[...] = s - times(alpha_re, alpha_im, q)
        return carry

    lax.fori_loop(0, jnp.minimum(steps, MR_MAX), step, 0)


def half_mask(shape, half):
    return low_half(shape) == (half == 0)


def messages(half, e, w_ref, mt_ref, mz_ref, back_slab, cd_ref, back_ref):
    place = lanes(e.shape) % (e.shape[-1] // 2)
    mz_ref[...] = jnp.where(place // PLANE == 0, e, w_ref[...])

    @pl.when(half == 0)
    def _():
        mt_ref[...] = e

    @pl.when(half != 0)
    def _():
        mt_ref[...] = backward_product(e, back_slab, cd_ref, back_ref)


def pack_rows(raw_re_im, half, write, dof):
    def body(row, carry):
        own = raw_re_im(half, row).astype(F32)
        other = raw_re_im(1 - half, row).astype(F32)
        write(row, jnp.where(half_mask(own.shape, half), own, swap(other)))
        return carry

    lax.fori_loop(0, dof, body, 0, unroll=4)


def which(colour):
    return (colour + lax.axis_index("sa")) % 2


def load_raw(links_ref, clover_ref, raw_ref, sem, order):
    copies = {}
    for term in order:
        source = clover_ref if term == 0 else links_ref.at[term % 4]
        copies[term] = pltpu.make_async_copy(source, raw_ref.at[term], sem.at[term])
        copies[term].start()
    return copies


def first_kernel(steps_ref, rhs_ref, links_ref, clover_ref, m_ref, time_ref, e_ref, s_ref, mt_ref, mz_ref,
                 raw_ref, sem, w_ref, ab_ref, cd_ref, back_ref, out_ref):
    dof = rhs_ref.shape[1]
    half = which(0)
    order = (0, 1, 2, 3, 4)
    copies = load_raw(links_ref, clover_ref, raw_ref, sem, order)
    own = rhs_ref[half]
    residual = jnp.where(half_mask(own.shape, half), own, swap(rhs_ref[1 - half]))
    for term in order:
        copies[term].wait()

        def write(row, packed, term=term):
            if term == 4:
                time_ref[row] = packed
            else:
                m_ref[term, row] = packed

        pack_rows(lambda part, row, term=term: raw_ref[term, part, row], 1 if term == 4 else half, write, dof)
    relax(residual, steps_ref[0, 0, half], m_ref, s_ref, e_ref, w_ref, ab_ref, cd_ref, back_ref, out_ref)
    messages(half, e_ref[...], w_ref, mt_ref, mz_ref, lambda row: time_ref[row], cd_ref, back_ref)


def local_part(half, e, base, time_get, r_ref, ab_ref, cd_ref, back_ref, out_ref):
    @pl.when(half == 0)
    def _():
        r_ref[...] = base() + backward_product(e, time_get, cd_ref, back_ref)

    @pl.when(half != 0)
    def _():
        spread_forward(e, ab_ref, 0)
        r_ref[...] = base() + forward_product([(time_get, 0)], ab_ref, out_ref, e.shape[0])


def second_kernel(rhs_ref, links_ref, clover_ref, e_ref, m_ref, time_ref, r_ref,
                  raw_ref, sem, ab_ref, cd_ref, back_ref, out_ref):
    dof = rhs_ref.shape[1]
    half = which(1)
    order = (4, 0, 1, 2, 3)
    copies = load_raw(links_ref, clover_ref, raw_ref, sem, order)
    for term in order:
        copies[term].wait()

        def write(row, packed, term=term):
            if term == 4:
                time_ref[row] = packed
            else:
                m_ref[term, row] = packed

        pack_rows(lambda part, row, term=term: raw_ref[term, part, row], 0 if term == 4 else half, write, dof)

    def base():
        own = rhs_ref[half]
        return jnp.where(half_mask(own.shape, half), own, swap(rhs_ref[1 - half]))

    local_part(1 - half, e_ref[...], base, lambda row: time_ref[row], r_ref, ab_ref, cd_ref, back_ref, out_ref)


def local_kernel(colour, e_ref, s_ref, time_ref, r_ref, ab_ref, cd_ref, back_ref, out_ref):
    half = which(colour)
    local_part(half, e_ref[...], lambda: s_ref[...], lambda row: time_ref[row], r_ref, ab_ref, cd_ref, back_ref, out_ref)


def remote_part(half, r, mt, mz_up, mz_down, m_ref, time_get, ab_ref, out_ref):
    dof, width = r.shape
    depth = lanes(r.shape) % (width // 2) // PLANE
    top = depth == LZ - 1
    spread_forward(jnp.where(top, turn(mz_up, (LZ - 1) * PLANE), 0.0), ab_ref, 0)
    spread_forward(jnp.where(half == 0, 0.0, mt), ab_ref, 1)
    total = r + jnp.where(depth == 0, turn(mz_down, -(LZ - 1) * PLANE), 0.0)
    total = total + jnp.where(half == 0, mt, 0.0)
    return total + forward_product([(lambda row: m_ref[1, row], 0), (time_get, 1)], ab_ref, out_ref, dof)


def sweep_kernel(colour, n_z, *refs):
    steps_ref, r_ref, mt_in, *refs = refs
    mz_in = refs[:n_z]
    m_ref, time_ref, sol_ref, *refs = refs[n_z:]
    e_ref, s_ref, new_ref, mt_ref, mz_ref, *refs = refs
    w_ref, ab_ref, cd_ref, back_ref, out_ref = refs
    half = which(colour)
    residual = remote_part(half, r_ref[...], mt_in[...], mz_in[0][...], mz_in[-1][...], m_ref,
                           lambda row: time_ref[row], ab_ref, out_ref)
    relax(residual, steps_ref[0, 0, half], m_ref, s_ref, e_ref, w_ref, ab_ref, cd_ref, back_ref, out_ref)
    messages(half, e_ref[...], w_ref, mt_ref, mz_ref, lambda row: time_ref[row], cd_ref, back_ref)
    new_ref[...] = sol_ref[...] + e_ref[...]


def unpack(half, block_here, block_other, out_ref):
    shape = block_here.shape
    low = low_half(shape)
    first = jnp.where(half == 0, block_here, block_other)
    second = jnp.where(half == 0, block_other, block_here)
    out_ref[0] = jnp.where(low, first, swap(second))
    out_ref[1] = jnp.where(low, swap(first), second)


def last_kernel(colour, n_z, *refs):
    r_ref, mt_in, *refs = refs
    mz_in = refs[:n_z]
    m_ref, time_ref, s_ref, x_here, x_other, *refs = refs[n_z:]
    sol_ref, res_ref, ab_ref, out_ref = refs
    half = which(colour)
    residual = remote_part(half, r_ref[...], mt_in[...], mz_in[0][...], mz_in[-1][...], m_ref,
                           lambda row: time_ref[row], ab_ref, out_ref)
    unpack(half, residual, s_ref[...], res_ref)
    unpack(half, x_here[...], x_other[...], sol_ref)


def shards(rhs, links, clover, mr_steps):
    dof = rhs.shape[2]
    width = rhs.shape[-1]
    rhs_local = rhs.reshape(2, dof, width)
    links_local = links.reshape(4, 2, dof, dof, width)
    clover_local = clover.reshape(2, dof, dof, width)
    n_t = lax.axis_size("ta")
    n_s = lax.axis_size("sa")
    n_z = 1 if n_s == 2 else 2

    vector = jax.ShapeDtypeStruct((dof, width), F32)
    slabs = jax.ShapeDtypeStruct((4, dof, dof, width), F32)
    slab = jax.ShapeDtypeStruct((dof, dof, width), F32)
    vec_scratch = pltpu.VMEM((dof, width), F32)
    ab = pltpu.VMEM((4, 2, dof, width), F32)
    cd = pltpu.VMEM((2, dof, width), F32)
    raw = pltpu.VMEM((5, 2, dof, dof, width), links.dtype)
    sems = pltpu.SemaphoreType.DMA((5,))
    params = pltpu.CompilerParams(vmem_limit_bytes=50 << 20)

    def exchange(colour, mt, mz):
        pairs = []
        for t in range(n_t):
            for s in range(n_s):
                goal = (t + 1) % n_t if (colour + s) % 2 else (t - 1) % n_t
                pairs.append((t * n_s + s, goal * n_s + s))
        mt_in = lax.ppermute(mt, ("ta", "sa"), pairs)
        down = [(s, (s - 1) % n_s) for s in range(n_s)]
        up = [(s, (s + 1) % n_s) for s in range(n_s)]
        mz_in = [lax.ppermute(mz, "sa", down)]
        if n_z == 2:
            mz_in.append(lax.ppermute(mz, "sa", up))
        return mt_in, mz_in

    m0, time1, e, s0, mt, mz = pl.pallas_call(
        first_kernel,
        in_specs=[SMEM, VMEM, ANY, ANY],
        out_specs=[VMEM] * 6,
        out_shape=[slabs, slab, vector, vector, vector, vector],
        scratch_shapes=[raw, sems, vec_scratch, ab, cd, ab, vec_scratch],
        compiler_params=params,
        name="first",
    )(mr_steps, rhs_local, links_local, clover_local)
    mt_in, mz_in = exchange(0, mt, mz)
    m1, time0, r = pl.pallas_call(
        second_kernel,
        in_specs=[VMEM, ANY, ANY, VMEM],
        out_specs=[VMEM] * 3,
        out_shape=[slabs, slab, vector],
        scratch_shapes=[raw, sems, ab, cd, ab, vec_scratch],
        compiler_params=params,
        name="second",
    )(rhs_local, links_local, clover_local, e)
    x = [e, None]
    blocks = [m0, m1]
    kept = [s0, None]
    last = 2 * SWEEPS - 1
    for index in range(1, last + 1):
        colour = index % 2
        e, kept[colour], x[colour], mt, mz = pl.pallas_call(
            functools.partial(sweep_kernel, colour, n_z),
            in_specs=[SMEM] + [VMEM] * (5 + n_z),
            out_specs=[VMEM] * 5,
            out_shape=[vector] * 5,
            scratch_shapes=[vec_scratch, ab, cd, ab, vec_scratch],
            compiler_params=params,
            name="sweep",
        )(mr_steps, r, mt_in, *mz_in, blocks[colour], time1, jnp.zeros_like(e) if x[colour] is None else x[colour])
        mt_in, mz_in = exchange(colour, mt, mz)
        r = pl.pallas_call(
            functools.partial(local_kernel, colour),
            in_specs=[VMEM] * 3,
            out_specs=VMEM,
            out_shape=vector,
            scratch_shapes=[ab, cd, ab, vec_scratch],
            compiler_params=params,
            name="local",
        )(e, kept[1 - colour], time0)
    colour = (last + 1) % 2
    pair = jax.ShapeDtypeStruct((2, dof, width), F32)
    sol, res = pl.pallas_call(
        functools.partial(last_kernel, colour, n_z),
        in_specs=[VMEM] * (7 + n_z),
        out_specs=[VMEM] * 2,
        out_shape=[pair, pair],
        scratch_shapes=[ab, vec_scratch],
        compiler_params=params,
        name="last",
    )(r, mt_in, *mz_in, blocks[colour], time1, kept[1 - colour], x[colour], x[1 - colour])
    return sol.reshape(rhs.shape), res.reshape(rhs.shape)


def solution(mesh):
    field = P(None, None, None, "ta", "sa", None)
    placed = (field, P(None, None, None, None, "ta", "sa", None), field, P("ta", "sa", None))
    return jax.shard_map(shards, mesh=mesh, in_specs=placed, out_specs=(field, field), check_vma=False)
```

```python
import functools

import jax
import jax.numpy as jnp
from jax import lax
from jax.experimental import pallas as pl
from jax.experimental.pallas import tpu as pltpu
from jax.sharding import PartitionSpec as P

LZ = 4
LY = 4
LX = 4
MR_MAX = 3
SWEEPS = 2
PLANE = LY * LX
UNIT = 4

F32 = jnp.float32
BF16 = jnp.bfloat16
VMEM = pl.BlockSpec(memory_space=pltpu.VMEM)
HBM = pl.BlockSpec(memory_space=pltpu.HBM)


def lanes(shape):
    return lax.broadcasted_iota(jnp.int32, shape, len(shape) - 1)


def sublanes(shape):
    return lax.broadcasted_iota(jnp.int32, shape, len(shape) - 2)


def low_half(shape):
    return lanes(shape) < shape[-1] // 2


def real_rows(shape):
    return sublanes(shape) % (2 * UNIT) < UNIT


def turn(x, amount):
    amount %= x.shape[-1]
    return pltpu.roll(x, amount, x.ndim - 1) if amount else x


def swap(x):
    return turn(x, x.shape[-1] // 2)


def tiles(x):
    return [x[k:k + 2 * UNIT] for k in range(0, x.shape[0], 2 * UNIT)]


def flip(x):
    return jnp.concatenate([pltpu.roll(t, UNIT, 0) for t in tiles(x)], 0)


def times_i(x):
    return jnp.where(real_rows(x.shape), -1.0, 1.0) * flip(x)


def chirality(shape):
    return jnp.where(low_half(shape), 1.0, -1.0).astype(F32)


def shifted(x, direction, sign, extra):
    place = lanes(x.shape) % (x.shape[-1] // 2)
    extent, stride = {1: (LZ, PLANE), 2: (LY, LX), 3: (LX, 1)}[direction]
    edge = place // stride % extent == (extent - 1 if sign > 0 else 0)
    inner = turn(x, extra - sign * stride)
    if direction == 1:
        return jnp.where(edge, 0.0, inner)
    return jnp.where(edge, turn(x, extra + sign * (extent - 1) * stride), inner)


def natural(x, y):
    low = low_half((2 * UNIT, x.shape[1]))
    real = real_rows(low.shape)
    pairs = list(zip(tiles(x), tiles(y)))
    units = [jnp.where(low, a, b) for a, b in pairs] + [jnp.where(low, b, a) for a, b in pairs]
    re, im = [], []
    for even, odd in zip(units[0::2], units[1::2]):
        re.append(jnp.where(real, even, pltpu.roll(odd, UNIT, 0)))
        im.append(jnp.where(real, pltpu.roll(even, UNIT, 0), odd))
    return jnp.concatenate(re, 0), jnp.concatenate(im, 0)


def unit_tiles(re, im):
    real = real_rows((2 * UNIT, re.shape[1]))
    out = []
    for a, b in zip(tiles(re), tiles(im)):
        out.append(jnp.where(real, a, pltpu.roll(b, UNIT, 0)))
        out.append(jnp.where(real, pltpu.roll(a, UNIT, 0), b))
    return out


def split(x):
    high = x.astype(BF16).astype(F32)
    return high, x - high


def gather_rows(parts):
    rows = sublanes(parts[0].shape)
    step = 1
    while len(parts) > 1:
        upper = (rows & step) != 0
        parts = [
            jnp.where(upper, odd, even) + pltpu.roll(jnp.where(upper, even, odd), step, 0)
            for even, odd in zip(parts[0::2], parts[1::2])
        ]
        step *= 2
    return parts[0]


def put_forward(x, y, ab_ref, slot):
    re, im = natural(x, y)
    for k, (r, i) in enumerate(zip(split(re), split(im))):
        ab_ref[slot, 0, k] = jnp.concatenate([r, -i], 0).astype(BF16)
        ab_ref[slot, 1, k] = jnp.concatenate([i, r], 0).astype(BF16)


def put_backward(x, rows_ref, spread_ref):
    dof, width = x.shape
    for k, part in enumerate(split(x * chirality(x.shape))):
        rows_ref[k] = part
        for row in range(dof):
            r, kind = UNIT * (row // (2 * UNIT)) + row % UNIT, row // UNIT % 2
            spread_ref[kind, k, r] = jnp.broadcast_to(rows_ref[k, row:row + 1, :], (16, width)).astype(BF16)


def forward_sums(terms, ab_ref, part_ref):
    entries, rows, width = terms[0][0].shape

    def body(group, carry):
        for own in range(2):
            r = 2 * group + own
            for kind in range(2):
                total = None
                for m_ref, slot in terms:
                    for t in range(0, rows, 16):
                        m = m_ref[r, pl.ds(t, 16), :].astype(F32)
                        for k in range(2):
                            product = m * ab_ref[slot, kind, k, pl.ds(t, 16), :].astype(F32)
                            total = product if total is None else total + product
                part_ref[kind, r] = total[:8] + total[8:]
        return carry

    lax.fori_loop(0, entries // 2, body, 0)
    out = []
    for t in range(0, entries, UNIT):
        parts = [part_ref[kind, t + k] for kind in range(2) for k in range(UNIT)]
        out.append(gather_rows(parts))
    return jnp.concatenate(out, 0)


def backward_sums(m_ref, spread_ref, back_ref):
    entries, rows, width = m_ref.shape
    starts = list(range(0, rows, 16))
    for pair in [starts[k:k + 2] for k in range(0, len(starts), 2)]:
        for t in pair:
            for kind in range(2):
                totals = [None] * (2 if len(pair) == 1 else 1)
                for r in range(entries):
                    m = m_ref[r, pl.ds(t, 16), :].astype(F32)
                    for k in range(2):
                        product = m * spread_ref[kind, k, r].astype(F32)
                        slot = k % len(totals)
                        totals[slot] = product if totals[slot] is None else totals[slot] + product
                back_ref[kind, pl.ds(t, 16), :] = totals[0] if len(totals) == 1 else totals[0] + totals[1]


def backward_halves(back_ref):
    dof = back_ref.shape[1] // 2
    re = back_ref[0, 0:dof, :] + back_ref[1, dof:2 * dof, :]
    im = back_ref[1, 0:dof, :] - back_ref[0, dof:2 * dof, :]
    units = unit_tiles(re, im)
    half = len(units) // 2
    low = low_half(units[0].shape)
    a = [jnp.where(low, p, q) for p, q in zip(units[:half], units[half:])]
    b = [jnp.where(low, q, p) for p, q in zip(units[:half], units[half:])]
    return jnp.concatenate(a, 0), jnp.concatenate(b, 0)


def block_operator(x, m_ref, ab_ref, rows_ref, spread_ref, back_ref, part_ref):
    half = x.shape[1] // 2
    put_forward(x, swap(x), ab_ref, 0)
    for direction in (1, 2, 3):
        put_forward(-shifted(x, direction, 1, 0), -shifted(x, direction, 1, half), ab_ref, direction)
    put_backward(x, rows_ref, spread_ref)

    def body(direction, carry):
        backward_sums(m_ref.at[direction], spread_ref, back_ref.at[direction])
        return carry

    lax.fori_loop(1, 4, body, 0)
    total = forward_sums([(m_ref.at[term], term) for term in range(4)], ab_ref, part_ref)
    backs = 0.0
    for direction in (1, 2, 3):
        a, b = backward_halves(back_ref.at[direction])
        backs = backs + shifted(a, direction, -1, 0) + shifted(b, direction, -1, half)
        if direction == 1:
            back_z = chirality(x.shape) * (a + swap(b))
    return total - chirality(x.shape) * backs, back_z


def backward_product(x, m_ref, rows_ref, spread_ref, back_ref):
    put_backward(x, rows_ref, spread_ref)
    backward_sums(m_ref, spread_ref, back_ref.at[0])
    a, b = backward_halves(back_ref.at[0])
    return chirality(x.shape) * (a + swap(b))


def total_of(x):
    return jnp.sum(jnp.sum(x, axis=0, keepdims=True), axis=1, keepdims=True)


def relax(residual, steps, m_ref, s_ref, e_ref, w_ref, work):
    s_ref[...] = residual
    e_ref[...] = jnp.zeros_like(residual)
    w_ref[...] = jnp.zeros_like(residual)

    def step(index, carry):
        s = s_ref[...]
        q, back_z = block_operator(s, m_ref, *work)
        s = s_ref[...]
        i_s = times_i(s)
        scale = total_of(q * q) + 1e-6
        live = index.astype(F32) < steps
        alpha_re = jnp.where(live, total_of(q * s) / scale, 0.0)
        alpha_im = jnp.where(live, -total_of(q * i_s) / scale, 0.0)
        e_ref[...] += alpha_re * s + alpha_im * i_s
        w_ref[...] += alpha_re * back_z + alpha_im * times_i(back_z)
        s_ref[...] = s - (alpha_re * q + alpha_im * times_i(q))
        return carry

    lax.fori_loop(0, MR_MAX, step, 0)


def send(half, e, w_ref, mt_ref, mz_ref, time_ref, rows_ref, spread_ref, back_ref):
    place = lanes(e.shape) % (e.shape[-1] // 2)
    mz_ref[...] = jnp.where(place // PLANE == 0, e, w_ref[...])

    @pl.when(half == 0)
    def _():
        mt_ref[...] = e

    @pl.when(half != 0)
    def _():
        mt_ref[...] = backward_product(e, time_ref, rows_ref, spread_ref, back_ref)


def half_mask(shape, half):
    return low_half(shape) == (half == 0)


def pack_matrix(raw_ref, half, own_ref, other_ref):
    dof = raw_ref.shape[1]
    entries = dof // 2
    mask = half_mask((dof, raw_ref.shape[-1]), half)

    def body(r, carry):
        for part in range(2):
            near = raw_ref[part, r + entries * half].astype(F32)
            far = raw_ref[part, r + entries * (1 - half)].astype(F32)
            own_ref[r, pl.ds(part * dof, dof), :] = jnp.where(mask, near, swap(far)).astype(BF16)
            other_ref[r, pl.ds(part * dof, dof), :] = jnp.where(mask, swap(near), far).astype(BF16)
        return carry

    lax.fori_loop(0, entries, body, 0, unroll=2)


def pack_field(ref, half):
    units = unit_tiles(ref[0], ref[1])
    count = len(units) // 2
    mask = half_mask(units[0].shape, half)
    first = jnp.concatenate(units[:count], 0)
    second = jnp.concatenate(units[count:], 0)
    own = jnp.where(half == 0, first, second)
    other = jnp.where(half == 0, second, first)
    return jnp.where(half_mask(own.shape, half), own, swap(other))


def unpack_fields(half, here, other, out_ref):
    first = natural(here, swap(here))
    second = natural(other, swap(other))
    for part in range(2):
        mask = half_mask(first[part].shape, half)
        out_ref[part] = jnp.where(mask, first[part], second[part])


def which(colour):
    return (colour + lax.axis_index("sa")) % 2


def fetch(pairs, sem):
    copies = [pltpu.make_async_copy(source, target, sem.at[k]) for k, (source, target) in enumerate(pairs)]
    for copy in copies:
        copy.start()
    return copies


def first_kernel(steps_in, rhs_in, links_in, clover_in, m_ref, time_ref, e_ref, s_ref, mt_ref, mz_ref, steps_ref,
                 m_other_ref, time_other_ref, r_ref, raw_ref, rhs_ref, count_ref, sem, w_ref, *work):
    half = which(0)
    pairs = [(rhs_in, rhs_ref), (steps_in, count_ref), (clover_in, raw_ref.at[0])]
    pairs += [(links_in.at[k % 4], raw_ref.at[k]) for k in (1, 2, 3, 4)]
    copies = fetch(pairs, sem)
    copies[0].wait()
    copies[1].wait()
    for k in range(2):
        steps_ref[k] = jnp.full(steps_ref.shape[1:], count_ref[0, 0, k].astype(F32))
    residual = pack_field(rhs_ref, half)
    r_ref[...] = pack_field(rhs_ref, 1 - half)
    for term in range(5):
        copies[2 + term].wait()
        if term == 4:
            pack_matrix(raw_ref.at[term], 1, time_ref, time_other_ref)
        else:
            pack_matrix(raw_ref.at[term], half, m_ref.at[term], m_other_ref.at[term])
    relax(residual, steps_ref[half, 0:1, 0:1], m_ref, s_ref, e_ref, w_ref, work)
    ab_ref, rows_ref, spread_ref, back_ref, part_ref = work
    send(half, e_ref[...], w_ref, mt_ref, mz_ref, time_ref, rows_ref, spread_ref, back_ref)


def local_part(half, e, base, time_ref, r_ref, ab_ref, rows_ref, spread_ref, back_ref, part_ref):
    @pl.when(half == 0)
    def _():
        r_ref[...] = base() + backward_product(e, time_ref, rows_ref, spread_ref, back_ref)

    @pl.when(half != 0)
    def _():
        put_forward(e, swap(e), ab_ref, 0)
        r_ref[...] = base() + forward_sums([(time_ref, 0)], ab_ref, part_ref)


def local_kernel(colour, e_ref, s_ref, time_ref, r_ref, *work):
    local_part(which(colour), e_ref[...], lambda: s_ref[...], time_ref, r_ref, *work)


def remote_part(half, r, mt, mz_up, mz_down, m_ref, time_ref, ab_ref, part_ref):
    depth = lanes(r.shape) % (r.shape[1] // 2) // PLANE
    reach = (LZ - 1) * PLANE
    top = depth == LZ - 1
    put_forward(jnp.where(top, turn(mz_up, reach), 0.0), jnp.where(top, turn(mz_up, reach + r.shape[1] // 2), 0.0), ab_ref, 0)
    ahead = jnp.where(half == 0, 0.0, mt)
    put_forward(ahead, swap(ahead), ab_ref, 1)
    total = r + jnp.where(depth == 0, turn(mz_down, -reach), 0.0) + jnp.where(half == 0, mt, 0.0)
    return total + forward_sums([(m_ref.at[1], 0), (time_ref, 1)], ab_ref, part_ref)


def sweep_kernel(colour, n_z, fresh, *refs):
    steps_ref, r_ref, mt_in, *refs = refs
    mz_in = refs[:n_z]
    m_ref, time_ref, *refs = refs[n_z:]
    if not fresh:
        sol_ref, *refs = refs
    e_ref, s_ref, new_ref, mt_ref, mz_ref, w_ref, *work = refs
    ab_ref, rows_ref, spread_ref, back_ref, part_ref = work
    half = which(colour)
    residual = remote_part(half, r_ref[...], mt_in[...], mz_in[0][...], mz_in[-1][...], m_ref, time_ref, ab_ref, part_ref)
    relax(residual, steps_ref[half, 0:1, 0:1], m_ref, s_ref, e_ref, w_ref, work)
    send(half, e_ref[...], w_ref, mt_ref, mz_ref, time_ref, rows_ref, spread_ref, back_ref)
    new_ref[...] = e_ref[...] if fresh else sol_ref[...] + e_ref[...]


def last_kernel(colour, n_z, *refs):
    r_ref, mt_in, *refs = refs
    mz_in = refs[:n_z]
    m_ref, time_ref, s_ref, x_here, x_other, sol_ref, res_ref, ab_ref, part_ref = refs[n_z:]
    half = which(colour)
    residual = remote_part(half, r_ref[...], mt_in[...], mz_in[0][...], mz_in[-1][...], m_ref, time_ref, ab_ref, part_ref)
    unpack_fields(half, residual, s_ref[...], res_ref)
    unpack_fields(half, x_here[...], x_other[...], sol_ref)


def shards(rhs, links, clover, mr_steps):
    dof = rhs.shape[2]
    width = rhs.shape[-1]
    rhs_local = rhs.reshape(2, dof, width)
    links_local = links.reshape(4, 2, dof, dof, width)
    clover_local = clover.reshape(2, dof, dof, width)
    n_t = lax.axis_size("ta")
    n_s = lax.axis_size("sa")
    n_z = 1 if n_s == 2 else 2

    vector = jax.ShapeDtypeStruct((dof, width), F32)
    matrix = jax.ShapeDtypeStruct((dof // 2, 2 * dof, width), BF16)
    matrices = jax.ShapeDtypeStruct((4,) + matrix.shape, BF16)
    counts = jax.ShapeDtypeStruct((2, 8, width), F32)
    pair = jax.ShapeDtypeStruct((2, dof, width), F32)
    field = pltpu.VMEM((dof, width), F32)
    ab = pltpu.VMEM((4, 2, 2, 2 * dof, width), BF16)
    part = pltpu.VMEM((2, dof // 2, 8, width), F32)
    work = [
        ab,
        pltpu.VMEM((2, dof, width), F32),
        pltpu.VMEM((2, 2, dof // 2, 16, width), BF16),
        pltpu.VMEM((4, 2, 2 * dof, width), F32),
        part,
    ]
    raw = pltpu.VMEM((5, 2, dof, dof, width), links.dtype)
    rhs_buffer = pltpu.VMEM((2, dof, width), F32)
    params = pltpu.CompilerParams(vmem_limit_bytes=20 << 20)

    def call(kernel, name, ins, outs, scratch):
        return pl.pallas_call(
            kernel,
            in_specs=ins,
            out_specs=[VMEM] * len(outs),
            out_shape=outs,
            scratch_shapes=scratch,
            compiler_params=params,
            name=name,
        )

    def exchange(colour, mt, mz):
        pairs = []
        for t in range(n_t):
            for s in range(n_s):
                goal = (t + 1) % n_t if (colour + s) % 2 else (t - 1) % n_t
                pairs.append((t * n_s + s, goal * n_s + s))
        mt_in = lax.ppermute(mt, ("ta", "sa"), pairs)
        mz_in = [lax.ppermute(mz, "sa", [(s, (s - 1) % n_s) for s in range(n_s)])]
        if n_z == 2:
            mz_in.append(lax.ppermute(mz, "sa", [(s, (s + 1) % n_s) for s in range(n_s)]))
        return mt_in, mz_in

    m0, time1, e, s0, mt, mz, steps, m1, time0, r = call(
        first_kernel, "first", [HBM] * 4,
        [matrices, matrix, vector, vector, vector, vector, counts, matrices, matrix, vector],
        [raw, rhs_buffer, pltpu.SMEM(mr_steps.shape, mr_steps.dtype), pltpu.SemaphoreType.DMA((7,)), field] + work,
    )(*[pltpu.with_memory_space_constraint(v, pltpu.HBM) for v in (mr_steps, rhs_local, links_local, clover_local)])

    def neighbours(colour, e, base):
        return call(functools.partial(local_kernel, colour), "local", [VMEM] * 3, [vector], work)(e, base, time0)[0]

    mt_in, mz_in = exchange(0, mt, mz)
    r = neighbours(0, e, r)
    blocks = [m0, m1]
    x = [e, None]
    kept = [s0, None]
    last = 2 * SWEEPS - 1
    for index in range(1, last + 1):
        colour = index % 2
        ins = [steps, r, mt_in, *mz_in, blocks[colour], time1]
        fresh = x[colour] is None
        if not fresh:
            ins.append(x[colour])
        e, kept[colour], x[colour], mt, mz = call(
            functools.partial(sweep_kernel, colour, n_z, fresh), "sweep", [VMEM] * len(ins), [vector] * 5, [field] + work
        )(*ins)
        mt_in, mz_in = exchange(colour, mt, mz)
        r = neighbours(colour, e, kept[1 - colour])
    colour = (last + 1) % 2
    ins = [r, mt_in, *mz_in, blocks[colour], time1, kept[1 - colour], x[colour], x[1 - colour]]
    sol, res = call(functools.partial(last_kernel, colour, n_z), "last", [VMEM] * len(ins), [pair, pair], [ab, part])(*ins)
    return sol.reshape(rhs.shape), res.reshape(rhs.shape)


def solution(mesh):
    field = P(None, None, None, "ta", "sa", None)
    placed = (field, P(None, None, None, None, "ta", "sa", None), field, P("ta", "sa", None))
    return jax.shard_map(shards, mesh=mesh, in_specs=placed, out_specs=(field, field), check_vma=False)
```

```python
import functools

import jax
import jax.numpy as jnp
from jax import lax
from jax.experimental import pallas as pl
from jax.experimental.pallas import tpu as pltpu
from jax.sharding import PartitionSpec as P


LZ = 4
LY = 4
LX = 4
MR_MAX = 3
SWEEPS = 2
PLANE = LY * LX
UNIT = 4
PIECES = 2

F32 = jnp.float32
BF16 = jnp.bfloat16
VMEM = pl.BlockSpec(memory_space=pltpu.VMEM)
HBM = pl.BlockSpec(memory_space=pltpu.HBM)


def lanes(shape):
    return lax.broadcasted_iota(jnp.int32, shape, len(shape) - 1)


def sublanes(shape):
    return lax.broadcasted_iota(jnp.int32, shape, len(shape) - 2)


def low_half(shape):
    return lanes(shape) < shape[-1] // 2


def real_rows(shape):
    return sublanes(shape) % (2 * UNIT) < UNIT


def turn(x, amount):
    amount %= x.shape[-1]
    return pltpu.roll(x, amount, x.ndim - 1) if amount else x


def swap(x):
    return turn(x, x.shape[-1] // 2)


def tiles(x):
    return [x[k:k + 2 * UNIT] for k in range(0, x.shape[0], 2 * UNIT)]


def flip(x):
    return jnp.concatenate([pltpu.roll(t, UNIT, 0) for t in tiles(x)], 0)


def times_i(x):
    return jnp.where(real_rows(x.shape), -1.0, 1.0) * flip(x)


def chirality(shape):
    return jnp.where(low_half(shape), 1.0, -1.0).astype(F32)


def shifted(x, direction, sign, extra):
    place = lanes(x.shape) % (x.shape[-1] // 2)
    extent, stride = {1: (LZ, PLANE), 2: (LY, LX), 3: (LX, 1)}[direction]
    edge = place // stride % extent == (extent - 1 if sign > 0 else 0)
    inner = turn(x, extra - sign * stride)
    if direction == 1:
        return jnp.where(edge, 0.0, inner)
    return jnp.where(edge, turn(x, extra + sign * (extent - 1) * stride), inner)


def natural(x, y):
    low = low_half((2 * UNIT, x.shape[1]))
    real = real_rows(low.shape)
    pairs = list(zip(tiles(x), tiles(y)))
    units = [jnp.where(low, a, b) for a, b in pairs] + [jnp.where(low, b, a) for a, b in pairs]
    re, im = [], []
    for even, odd in zip(units[0::2], units[1::2]):
        re.append(jnp.where(real, even, pltpu.roll(odd, UNIT, 0)))
        im.append(jnp.where(real, pltpu.roll(even, UNIT, 0), odd))
    return jnp.concatenate(re, 0), jnp.concatenate(im, 0)


def unit_tiles(re, im):
    real = real_rows((2 * UNIT, re.shape[1]))
    out = []
    for a, b in zip(tiles(re), tiles(im)):
        out.append(jnp.where(real, a, pltpu.roll(b, UNIT, 0)))
        out.append(jnp.where(real, pltpu.roll(a, UNIT, 0), b))
    return out


def split(x):
    high = x.astype(BF16).astype(F32)
    return high, x - high


def gather_rows(parts):
    rows = sublanes(parts[0].shape)
    step = 1
    while len(parts) > 1:
        upper = (rows & step) != 0
        parts = [
            jnp.where(upper, odd, even) + pltpu.roll(jnp.where(upper, even, odd), step, 0)
            for even, odd in zip(parts[0::2], parts[1::2])
        ]
        step *= 2
    return parts[0]


def put_forward(x, y, ab_ref, slot):
    re, im = natural(x, y)
    for k, (r, i) in enumerate(zip(split(re), split(im))):
        ab_ref[slot, 0, k] = jnp.concatenate([r, -i], 0).astype(BF16)
        ab_ref[slot, 1, k] = jnp.concatenate([i, r], 0).astype(BF16)


def put_backward(x, rows_ref, spread_ref):
    dof, width = x.shape
    for k, part in enumerate(split(x * chirality(x.shape))):
        rows_ref[k] = part
        for row in range(dof):
            r, kind = UNIT * (row // (2 * UNIT)) + row % UNIT, row // UNIT % 2
            spread_ref[kind, k, r] = jnp.broadcast_to(rows_ref[k, row:row + 1, :], (16, width)).astype(BF16)


def forward_sums(terms, ab_ref, part_ref, unroll=1):
    entries, rows, _ = terms[0][0].shape

    def body(group, carry):
        for own in range(2):
            r = 2 * group + own
            for kind in range(2):
                total = None
                for m_ref, slot in terms:
                    for t in range(0, rows, 16):
                        m = m_ref[r, pl.ds(t, 16), :].astype(F32)
                        for k in range(2):
                            product = m * ab_ref[slot, kind, k, pl.ds(t, 16), :].astype(F32)
                            total = product if total is None else total + product
                part_ref[kind, r] = total[:8] + total[8:]
        return carry

    lax.fori_loop(0, entries // 2, body, 0, unroll=unroll)
    out = []
    for t in range(0, entries, UNIT):
        parts = [part_ref[kind, t + k] for kind in range(2) for k in range(UNIT)]
        out.append(gather_rows(parts))
    return jnp.concatenate(out, 0)


def backward_sums(m_ref, spread_ref, back_ref):
    entries, rows, _ = m_ref.shape
    starts = list(range(0, rows, 16))
    for pair in [starts[k:k + 2] for k in range(0, len(starts), 2)]:
        for t in pair:
            for kind in range(2):
                totals = [None] * (2 if len(pair) == 1 else 1)
                for r in range(entries):
                    m = m_ref[r, pl.ds(t, 16), :].astype(F32)
                    for k in range(2):
                        product = m * spread_ref[kind, k, r].astype(F32)
                        slot = k % len(totals)
                        totals[slot] = product if totals[slot] is None else totals[slot] + product
                back_ref[kind, pl.ds(t, 16), :] = totals[0] if len(totals) == 1 else totals[0] + totals[1]


def backward_halves(back_ref):
    dof = back_ref.shape[1] // 2
    re = back_ref[0, 0:dof, :] + back_ref[1, dof:2 * dof, :]
    im = back_ref[1, 0:dof, :] - back_ref[0, dof:2 * dof, :]
    units = unit_tiles(re, im)
    half = len(units) // 2
    low = low_half(units[0].shape)
    a = [jnp.where(low, p, q) for p, q in zip(units[:half], units[half:])]
    b = [jnp.where(low, q, p) for p, q in zip(units[:half], units[half:])]
    return jnp.concatenate(a, 0), jnp.concatenate(b, 0)


def block_operator(x, unroll, m_ref, ab_ref, rows_ref, spread_ref, back_ref, part_ref):
    half = x.shape[1] // 2
    put_forward(x, swap(x), ab_ref, 0)
    for direction in (1, 2, 3):
        put_forward(-shifted(x, direction, 1, 0), -shifted(x, direction, 1, half), ab_ref, direction)
    put_backward(x, rows_ref, spread_ref)

    for direction in (1, 2, 3):
        backward_sums(m_ref.at[direction], spread_ref, back_ref.at[direction])
    total = forward_sums([(m_ref.at[term], term) for term in range(4)], ab_ref, part_ref, unroll)
    backs = 0.0
    for direction in (1, 2, 3):
        a, b = backward_halves(back_ref.at[direction])
        backs = backs + shifted(a, direction, -1, 0) + shifted(b, direction, -1, half)
        if direction == 1:
            back_z = chirality(x.shape) * (a + swap(b))
    return total - chirality(x.shape) * backs, back_z


def backward_product(x, m_ref, rows_ref, spread_ref, back_ref):
    put_backward(x, rows_ref, spread_ref)
    backward_sums(m_ref, spread_ref, back_ref.at[0])
    a, b = backward_halves(back_ref.at[0])
    return chirality(x.shape) * (a + swap(b))


def total_of(x):
    parts = tiles(x)
    total = parts[0]
    for part in parts[1:]:
        total = total + part
    for amount in (4, 2, 1):
        total = total + pltpu.roll(total, amount, 0)
    return jnp.broadcast_to(jnp.sum(total, axis=1, keepdims=True), total.shape)


def scaled(alpha, x):
    return jnp.concatenate([alpha * tile for tile in tiles(x)], 0)


def relax(residual, steps, m_ref, s_ref, e_ref, w_ref, work, mine=None):
    @pl.when(True if mine is None else mine)
    def _():
        s_ref[...] = residual
        e_ref[...] = jnp.zeros_like(residual)
        w_ref[...] = jnp.zeros_like(residual)

    def step(index, carry):
        s = s_ref[...]
        q, back_z = block_operator(s, s.shape[0] // (4 if mine is None else 8), m_ref, *work)
        s = s_ref[...]
        i_s = times_i(s)
        scale = total_of(q * q) + 1e-6
        live = index.astype(F32) < steps
        alpha_re = jnp.where(live, total_of(q * s) / scale, 0.0)
        alpha_im = jnp.where(live, -total_of(q * i_s) / scale, 0.0)
        e_ref[...] += scaled(alpha_re, s) + scaled(alpha_im, i_s)
        w_ref[...] += scaled(alpha_re, back_z) + scaled(alpha_im, times_i(back_z))
        s_ref[...] = s - (scaled(alpha_re, q) + scaled(alpha_im, times_i(q)))
        return carry

    lax.fori_loop(0, MR_MAX if mine is None else jnp.where(mine, MR_MAX, 0), step, 0)


def send(half, e, w_ref, mt_ref, mz_ref, time_ref, rows_ref, spread_ref, back_ref):
    place = lanes(e.shape) % (e.shape[-1] // 2)
    mz_ref[...] = jnp.where(place // PLANE == 0, e, w_ref[...])

    @pl.when(half == 0)
    def _():
        mt_ref[...] = e

    @pl.when(half != 0)
    def _():
        mt_ref[...] = backward_product(e, time_ref, rows_ref, spread_ref, back_ref)


def half_mask(shape, half):
    return low_half(shape) == (half == 0)


def pack_matrix(raw_ref, half, own_ref, other_ref):
    dof = raw_ref.shape[1]
    entries = dof // 2
    mask = half_mask((dof, raw_ref.shape[-1]), half)

    def body(r, carry):
        for part in range(2):
            near = raw_ref[part, r + entries * half].astype(F32)
            far = raw_ref[part, r + entries * (1 - half)].astype(F32)
            own_ref[r, pl.ds(part * dof, dof), :] = jnp.where(mask, near, swap(far)).astype(BF16)
            other_ref[r, pl.ds(part * dof, dof), :] = jnp.where(mask, swap(near), far).astype(BF16)
        return carry

    lax.fori_loop(0, entries, body, 0, unroll=10)


def pack_field(ref, half):
    units = unit_tiles(ref[0], ref[1])
    count = len(units) // 2
    mask = half_mask(units[0].shape, half)
    first = jnp.concatenate(units[:count], 0)
    second = jnp.concatenate(units[count:], 0)
    own = jnp.where(half == 0, first, second)
    other = jnp.where(half == 0, second, first)
    return jnp.where(half_mask(own.shape, half), own, swap(other))


def unpack_fields(half, here, other, out_ref):
    first = natural(here, swap(here))
    second = natural(other, swap(other))
    for part in range(2):
        mask = half_mask(first[part].shape, half)
        out_ref[part] = jnp.where(mask, first[part], second[part])


def which(colour):
    return (colour + lax.axis_index("sa")) % 2


def fetch(pairs, sem):
    copies = [pltpu.make_async_copy(source, target, sem.at[k]) for k, (source, target) in enumerate(pairs)]
    for copy in copies:
        copy.start()
    return copies


def first_turn(late):
    early = lax.axis_index("ta") % 2 == which(0)
    return jnp.logical_not(early) if late else early


def pack_kernel(late, *refs):
    steps_in, rhs_in, links_in, clover_in, *refs = refs
    if late:
        refs = refs[7:]
    (m_ref, time_ref, m_other_ref, time_other_ref, own_ref, other_ref, steps_ref,
     raw_ref, rhs_ref, count_ref, sem) = refs
    half = which(0)

    @pl.when(first_turn(late))
    def _():
        dof = rhs_ref.shape[1]
        pieces = []
        for term in range(5):
            source = clover_in if term == 0 else links_in.at[term % 4]
            for part in range(2):
                for row in range(0, dof, dof // PIECES):
                    rows = pl.ds(row, dof // PIECES)
                    pieces.append((source.at[part, rows], raw_ref.at[term, part, rows]))
        copies = fetch(pieces + [(rhs_in, rhs_ref), (steps_in, count_ref)], sem)
        for term in range(5):
            for copy in copies[2 * PIECES * term:2 * PIECES * (term + 1)]:
                copy.wait()
            if term == 4:
                pack_matrix(raw_ref.at[term], 1, time_ref, time_other_ref)
            else:
                pack_matrix(raw_ref.at[term], half, m_ref.at[term], m_other_ref.at[term])
        copies[-2].wait()
        copies[-1].wait()
        for k in range(2):
            steps_ref[k] = jnp.full(steps_ref.shape[1:], count_ref[0, 0, k].astype(F32))
        own_ref[...] = pack_field(rhs_ref, half)
        other_ref[...] = pack_field(rhs_ref, 1 - half)


def first_kernel(late, steps_ref, r_ref, m_ref, time_ref, *refs):
    if late:
        refs = refs[3:]
    e_ref, s_ref, mz_ref, mt_ref, w_ref, *work = refs
    _, rows_ref, spread_ref, back_ref, _ = work
    half = which(0)
    mine = first_turn(late)
    relax(r_ref[...], steps_ref[half], m_ref, s_ref, e_ref, w_ref, work, mine)

    @pl.when(mine)
    def _():
        send(half, e_ref[...], w_ref, mt_ref, mz_ref, time_ref, rows_ref, spread_ref, back_ref)


def local_part(half, e, base, time_ref, r_ref, ab_ref, rows_ref, spread_ref, back_ref, part_ref):
    @pl.when(half == 0)
    def _():
        r_ref[...] = base() + backward_product(e, time_ref, rows_ref, spread_ref, back_ref)

    @pl.when(half != 0)
    def _():
        put_forward(e, swap(e), ab_ref, 0)
        r_ref[...] = base() + forward_sums([(time_ref, 0)], ab_ref, part_ref)


def local_kernel(colour, e_ref, s_ref, time_ref, *refs):
    half = which(colour)
    if len(refs) > 6:
        x_here, x_other, r_ref, sol_ref, *work = refs
        unpack_fields(half, x_here[...], x_other[...], sol_ref)
    else:
        r_ref, *work = refs
    local_part(half, e_ref[...], lambda: s_ref[...], time_ref, r_ref, *work)


def remote_part(half, r, mt, mz_up, mz_down, m_ref, time_ref, ab_ref, part_ref):
    depth = lanes(r.shape) % (r.shape[1] // 2) // PLANE
    reach = (LZ - 1) * PLANE
    top = depth == LZ - 1
    put_forward(jnp.where(top, turn(mz_up, reach), 0.0), jnp.where(top, turn(mz_up, reach + r.shape[1] // 2), 0.0), ab_ref, 0)
    ahead = jnp.where(half == 0, 0.0, mt)
    put_forward(ahead, swap(ahead), ab_ref, 1)
    total = r + jnp.where(depth == 0, turn(mz_down, -reach), 0.0) + jnp.where(half == 0, mt, 0.0)
    return total + forward_sums([(m_ref.at[1], 0), (time_ref, 1)], ab_ref, part_ref)


def sweep_kernel(colour, n_t_in, n_z, fresh, *refs):
    steps_ref, r_ref, *refs = refs
    mt, mz_up, mz_down, refs = arrivals(refs, n_t_in, n_z)
    m_ref, time_ref, *refs = refs
    if not fresh:
        sol_ref, *refs = refs
    e_ref, s_ref, new_ref, mz_ref, mt_ref, w_ref, *work = refs
    ab_ref, rows_ref, spread_ref, back_ref, part_ref = work
    half = which(colour)
    residual = remote_part(half, r_ref[...], mt, mz_up, mz_down, m_ref, time_ref, ab_ref, part_ref)
    relax(residual, steps_ref[half], m_ref, s_ref, e_ref, w_ref, work)
    send(half, e_ref[...], w_ref, mt_ref, mz_ref, time_ref, rows_ref, spread_ref, back_ref)
    new_ref[...] = e_ref[...] if fresh else sol_ref[...] + e_ref[...]


def arrivals(refs, n_t_in, n_z):
    mt = refs[0][...]
    if n_t_in == 2:
        mt = jnp.where(first_turn(False), refs[1][...], mt)
    up, down = refs[n_t_in], refs[n_t_in + n_z - 1]
    return mt, up[...], down[...], refs[n_t_in + n_z:]


def last_kernel(colour, n_z, r_ref, *refs):
    mt, mz_up, mz_down, refs = arrivals(refs, 1, n_z)
    m_ref, time_ref, s_ref, res_ref, ab_ref, part_ref = refs
    half = which(colour)
    residual = remote_part(half, r_ref[...], mt, mz_up, mz_down, m_ref, time_ref, ab_ref, part_ref)
    unpack_fields(half, residual, s_ref[...], res_ref)


def shards(rhs, links, clover, mr_steps):
    dof = rhs.shape[2]
    width = rhs.shape[-1]
    rhs_local = rhs.reshape(2, dof, width)
    links_local = links.reshape(4, 2, dof, dof, width)
    clover_local = clover.reshape(2, dof, dof, width)
    n_t = lax.axis_size("ta")
    n_s = lax.axis_size("sa")
    n_z = 1 if n_s == 2 else 2

    vector = jax.ShapeDtypeStruct((dof, width), F32)
    matrix = jax.ShapeDtypeStruct((dof // 2, 2 * dof, width), BF16)
    matrices = jax.ShapeDtypeStruct((4,) + matrix.shape, BF16)
    counts = jax.ShapeDtypeStruct((2, 8, width), F32)
    pair = jax.ShapeDtypeStruct((2, dof, width), F32)
    field = pltpu.VMEM((dof, width), F32)
    ab = pltpu.VMEM((4, 2, 2, 2 * dof, width), BF16)
    part = pltpu.VMEM((2, dof // 2, 8, width), F32)
    work = [
        ab,
        pltpu.VMEM((2, dof, width), F32),
        pltpu.VMEM((2, 2, dof // 2, 16, width), BF16),
        pltpu.VMEM((4, 2, 2 * dof, width), F32),
        part,
    ]
    raw = pltpu.VMEM((5, 2, dof, dof, width), links.dtype)
    rhs_buffer = pltpu.VMEM((2, dof, width), F32)
    params = pltpu.CompilerParams(vmem_limit_bytes=20 << 20)

    def call(kernel, ins, outs, scratch, specs=None, aliases={}):
        return pl.pallas_call(
            kernel,
            in_specs=specs or [VMEM] * len(ins),
            out_specs=[VMEM] * len(outs),
            out_shape=outs,
            scratch_shapes=scratch,
            compiler_params=params,
            input_output_aliases=aliases,
        )(*ins)

    def time_pairs(colour, late=None):
        pairs = []
        for t in range(n_t):
            for s in range(n_s):
                half = (colour + s) % 2
                if late is None or (t % 2 != half) == late:
                    goal = (t + 1) % n_t if half else (t - 1) % n_t
                    pairs.append((t * n_s + s, goal * n_s + s))
                elif late and n_s % 2 == 0 and n_t % 2 == 0:
                    pairs.append((t * n_s + s, t * n_s + (s + 1) % n_s))
        return pairs

    def along_time(mt, colour, late=None):
        return lax.ppermute(mt, ("ta", "sa"), time_pairs(colour, late))

    def along_z(mz):
        got = [lax.ppermute(mz, "sa", [(s, (s - 1) % n_s) for s in range(n_s)])]
        if n_z == 2:
            got.append(lax.ppermute(mz, "sa", [(s, (s + 1) % n_s) for s in range(n_s)]))
        return got

    args = [pltpu.with_memory_space_constraint(v, pltpu.HBM) for v in (mr_steps, rhs_local, links_local, clover_local)]
    outs = [matrices, matrix, matrices, matrix, vector, vector, counts]
    scratch = [raw, rhs_buffer, pltpu.SMEM(mr_steps.shape, mr_steps.dtype), pltpu.SemaphoreType.DMA((10 * PIECES + 2,))]
    packed = call(functools.partial(pack_kernel, False), args, outs, scratch, [HBM] * 4)
    m0, time1, m1, time0, own, r, steps = packed
    early = call(functools.partial(first_kernel, False), [steps, own, m0, time1], [vector] * 4, [field] + work)
    mt_a = along_time(early[-1], 0, False)
    m0, time1, m1, time0, own, r, steps = call(
        functools.partial(pack_kernel, True), [*args, *packed], outs, scratch,
        [HBM] * 4 + [VMEM] * 7, {4 + k: k for k in range(7)},
    )
    e, s0, mz, mt = call(
        functools.partial(first_kernel, True), [steps, own, m0, time1, *early[:-1]], [vector] * 4,
        [field] + work, None, {4 + k: k for k in range(3)},
    )
    got = [mt_a, along_time(mt, 0, True), *along_z(mz)]

    def neighbours(colour, e, base, fields=()):
        outs = [vector, pair] if fields else [vector]
        return call(functools.partial(local_kernel, colour), [e, base, time0, *fields], outs, work)

    (r,) = neighbours(0, e, r)
    blocks = [m0, m1]
    x = [e, None]
    kept = [s0, None]
    last = 2 * SWEEPS - 1
    for index in range(1, last + 1):
        colour = index % 2
        ins = [steps, r, *got, blocks[colour], time1]
        fresh = x[colour] is None
        if not fresh:
            ins.append(x[colour])
        kernel = functools.partial(sweep_kernel, colour, len(got) - n_z, n_z, fresh)
        e, kept[colour], x[colour], mz, mt = call(kernel, ins, [vector] * 5, [field] + work)
        got = [along_time(mt, colour), *along_z(mz)]
        fields = (x[colour], x[1 - colour]) if index == last else ()
        r, *sol = neighbours(colour, e, kept[1 - colour], fields)
    colour = (last + 1) % 2
    ins = [r, *got, blocks[colour], time1, kept[1 - colour]]
    (res,) = call(functools.partial(last_kernel, colour, n_z), ins, [pair], [ab, part])
    return sol[0].reshape(rhs.shape), res.reshape(rhs.shape)


def solution(mesh):
    field = P(None, None, None, "ta", "sa", None)
    placed = (field, P(None, None, None, None, "ta", "sa", None), field, P("ta", "sa", None))
    return jax.shard_map(shards, mesh=mesh, in_specs=placed, out_specs=(field, field), check_vma=False)
```

```python
import functools

import jax
import jax.numpy as jnp
from jax import lax
from jax.experimental import pallas as pl
from jax.experimental.pallas import tpu as pltpu
from jax.sharding import PartitionSpec as P


LZ = 4
LY = 4
LX = 4
MR_MAX = 3
SWEEPS = 2
PLANE = LY * LX
UNIT = 4
PIECES = 1

F32 = jnp.float32
BF16 = jnp.bfloat16
VMEM = pl.BlockSpec(memory_space=pltpu.VMEM)
HBM = pl.BlockSpec(memory_space=pltpu.HBM)


def lanes(shape):
    return lax.broadcasted_iota(jnp.int32, shape, len(shape) - 1)


def sublanes(shape):
    return lax.broadcasted_iota(jnp.int32, shape, len(shape) - 2)


def low_half(shape):
    return lanes(shape) < shape[-1] // 2


def real_rows(shape):
    return sublanes(shape) % (2 * UNIT) < UNIT


def turn(x, amount):
    amount %= x.shape[-1]
    return pltpu.roll(x, amount, x.ndim - 1) if amount else x


def swap(x):
    return turn(x, x.shape[-1] // 2)


def tiles(x):
    return [x[k:k + 2 * UNIT] for k in range(0, x.shape[0], 2 * UNIT)]


def flip(x):
    return jnp.concatenate([pltpu.roll(t, UNIT, 0) for t in tiles(x)], 0)


def times_i(x):
    return jnp.where(real_rows(x.shape), -1.0, 1.0) * flip(x)


def chirality(shape):
    return jnp.where(low_half(shape), 1.0, -1.0).astype(F32)


def shifted(x, direction, sign, extra):
    place = lanes(x.shape) % (x.shape[-1] // 2)
    extent, stride = {1: (LZ, PLANE), 2: (LY, LX), 3: (LX, 1)}[direction]
    edge = place // stride % extent == (extent - 1 if sign > 0 else 0)
    inner = turn(x, extra - sign * stride)
    if direction == 1:
        return jnp.where(edge, jnp.zeros_like(inner), inner)
    return jnp.where(edge, turn(x, extra + sign * (extent - 1) * stride), inner)


def natural(x, y):
    low = low_half((2 * UNIT, x.shape[1]))
    real = real_rows(low.shape)
    pairs = list(zip(tiles(x), tiles(y)))
    units = [jnp.where(low, a, b) for a, b in pairs] + [jnp.where(low, b, a) for a, b in pairs]
    re, im = [], []
    for even, odd in zip(units[0::2], units[1::2]):
        re.append(jnp.where(real, even, pltpu.roll(odd, UNIT, 0)))
        im.append(jnp.where(real, pltpu.roll(even, UNIT, 0), odd))
    return jnp.concatenate(re, 0), jnp.concatenate(im, 0)


def unit_tiles(re, im):
    real = real_rows((2 * UNIT, re.shape[1]))
    out = []
    for a, b in zip(tiles(re), tiles(im)):
        out.append(jnp.where(real, a, pltpu.roll(b, UNIT, 0)))
        out.append(jnp.where(real, pltpu.roll(a, UNIT, 0), b))
    return out


def split(x):
    high = x.astype(BF16).astype(F32)
    return high, x - high


def gather_rows(parts):
    rows = sublanes(parts[0].shape)
    step = 1
    while len(parts) > 1:
        upper = (rows & step) != 0
        parts = [
            jnp.where(upper, odd, even) + pltpu.roll(jnp.where(upper, even, odd), step, 0)
            for even, odd in zip(parts[0::2], parts[1::2])
        ]
        step *= 2
    return parts[0]


def put_forward(x, y, ab_ref, slot):
    re, im = natural(x, y)
    for k, (r, i) in enumerate(zip(split(re), split(im))):
        ab_ref[slot, 0, k] = jnp.concatenate([r, -i], 0).astype(BF16)
        ab_ref[slot, 1, k] = jnp.concatenate([i, r], 0).astype(BF16)


def put_backward(x, rows_ref, spread_ref):
    dof, width = x.shape
    for k, part in enumerate(split(x * chirality(x.shape))):
        rows_ref[k] = part
        for row in range(dof):
            r, kind = UNIT * (row // (2 * UNIT)) + row % UNIT, row // UNIT % 2
            spread_ref[kind, k, r] = jnp.broadcast_to(rows_ref[k, row:row + 1, :], (16, width)).astype(BF16)


def forward_sums(terms, ab_ref, part_ref, unroll=1, start=0):
    entries, rows, _ = terms[0][0].shape

    def body(group, carry):
        for own in range(2):
            r = 2 * group + own
            for kind in range(2):
                total = None
                for m_ref, slot in terms:
                    for t in range(0, rows, 16):
                        m = m_ref[r + start, pl.ds(t, 16), :].astype(F32)
                        for k in range(2):
                            product = m * ab_ref[slot, kind, k, pl.ds(t, 16), :].astype(F32)
                            total = product if total is None else total + product
                part_ref[kind, r] = total
        return carry

    lax.fori_loop(0, entries // 2, body, 0, unroll=unroll)
    out = []
    for t in range(0, entries, UNIT):
        parts = [part_ref[kind, t + k, 0:8, :] + part_ref[kind, t + k, 8:16, :] for kind in range(2) for k in range(UNIT)]
        out.append(gather_rows(parts))
    return jnp.concatenate(out, 0)


def backward_sums(m_ref, spread_ref, back_ref):
    entries, rows, _ = m_ref.shape
    for t in range(0, rows, 16):
        for kind in range(2):
            total = None
            for r in range(entries):
                m = m_ref[r, pl.ds(t, 16), :].astype(F32)
                for k in range(2):
                    product = m * spread_ref[kind, k, r].astype(F32)
                    total = product if total is None else total + product
            back_ref[kind, pl.ds(t, 16), :] = total


def backward_halves(back_ref):
    dof = back_ref.shape[1] // 2
    re = back_ref[0, 0:dof, :] + back_ref[1, dof:2 * dof, :]
    im = back_ref[1, 0:dof, :] - back_ref[0, dof:2 * dof, :]
    units = unit_tiles(re, im)
    half = len(units) // 2
    low = low_half(units[0].shape)
    a = [jnp.where(low, p, q) for p, q in zip(units[:half], units[half:])]
    b = [jnp.where(low, q, p) for p, q in zip(units[:half], units[half:])]
    return jnp.concatenate(a, 0), jnp.concatenate(b, 0)


def block_operator(x, unroll, start, m_ref, ab_ref, rows_ref, spread_ref, back_ref, part_ref):
    half = x.shape[1] // 2
    put_forward(x, swap(x), ab_ref, 0)
    for kind in range(2):
        for k in range(2):
            hopped = -ab_ref[0, kind, k]
            for direction in (1, 2, 3):
                ab_ref[direction, kind, k] = shifted(hopped, direction, 1, 0)
    put_backward(x, rows_ref, spread_ref)

    for direction in (1, 2, 3):
        backward_sums(m_ref.at[direction], spread_ref, back_ref.at[direction])
    total = forward_sums([(m_ref.at[term], term) for term in range(4)], ab_ref, part_ref, unroll, start)
    backs = 0.0
    for direction in (1, 2, 3):
        a, b = backward_halves(back_ref.at[direction])
        backs = backs + shifted(a, direction, -1, 0) + shifted(b, direction, -1, half)
        if direction == 1:
            back_z = chirality(x.shape) * (a + swap(b))
    return total - chirality(x.shape) * backs, back_z


def backward_product(x, m_ref, rows_ref, spread_ref, back_ref):
    put_backward(x, rows_ref, spread_ref)
    backward_sums(m_ref, spread_ref, back_ref.at[0])
    a, b = backward_halves(back_ref.at[0])
    return chirality(x.shape) * (a + swap(b))


def total_of(x):
    parts = tiles(x)
    total = parts[0]
    for part in parts[1:]:
        total = total + part
    for amount in (4, 2, 1):
        total = total + pltpu.roll(total, amount, 0)
    return jnp.broadcast_to(jnp.sum(total, axis=1, keepdims=True), total.shape)


def scaled(alpha, x):
    return jnp.concatenate([alpha * tile for tile in tiles(x)], 0)


def relax(residual, steps, m_ref, s_ref, e_ref, w_ref, work, mine=None, trips=4):
    @pl.when(True if mine is None else mine)
    def _():
        if residual is not None:
            s_ref[...] = residual
        e_ref[...] = jnp.zeros_like(e_ref)
        w_ref[...] = jnp.zeros_like(w_ref)

    def step(index, carry):
        s = s_ref[...]
        q, back_z = block_operator(s, s.shape[0] // trips, jnp.minimum(index, 0), m_ref, *work)
        s = s_ref[...]
        i_s = times_i(s)
        scale = total_of(q * q) + 1e-6
        live = index.astype(F32) < steps
        alpha_re = jnp.where(live, total_of(q * s) / scale, 0.0)
        alpha_im = jnp.where(live, -total_of(q * i_s) / scale, 0.0)
        e_ref[...] += scaled(alpha_re, s) + scaled(alpha_im, i_s)
        w_ref[...] += scaled(alpha_re, back_z) + scaled(alpha_im, times_i(back_z))
        s_ref[...] = s - (scaled(alpha_re, q) + scaled(alpha_im, times_i(q)))
        return carry

    lax.fori_loop(0, MR_MAX if mine is None else jnp.where(mine, MR_MAX, 0), step, 0)


def send(half, e, w_ref, mt_ref, mz_ref, time_ref, rows_ref, spread_ref, back_ref):
    place = lanes(e.shape) % (e.shape[-1] // 2)
    mz_ref[...] = jnp.where(place // PLANE == 0, e, w_ref[...])

    @pl.when(half == 0)
    def _():
        mt_ref[...] = e

    @pl.when(half != 0)
    def _():
        mt_ref[...] = backward_product(e, time_ref, rows_ref, spread_ref, back_ref)


def half_mask(shape, half):
    return low_half(shape) == (half == 0)


def pack_matrix(raw_ref, half, own_ref, other_ref):
    dof = raw_ref.shape[1]
    entries = dof // 2
    mask = half_mask((dof, raw_ref.shape[-1]), half)

    def body(r, carry):
        for part in range(2):
            near = raw_ref[part, r + entries * half].astype(F32)
            far = raw_ref[part, r + entries * (1 - half)].astype(F32)
            own_ref[r, pl.ds(part * dof, dof), :] = jnp.where(mask, near, swap(far)).astype(BF16)
            other_ref[r, pl.ds(part * dof, dof), :] = jnp.where(mask, swap(near), far).astype(BF16)
        return carry

    lax.fori_loop(0, entries, body, 0, unroll=10)


def pack_field(ref, half):
    units = unit_tiles(ref[0], ref[1])
    count = len(units) // 2
    mask = half_mask(units[0].shape, half)
    first = jnp.concatenate(units[:count], 0)
    second = jnp.concatenate(units[count:], 0)
    own = jnp.where(half == 0, first, second)
    other = jnp.where(half == 0, second, first)
    return jnp.where(half_mask(own.shape, half), own, swap(other))


def unpack_fields(half, here, other, out_ref):
    first = natural(here, swap(here))
    second = natural(other, swap(other))
    for part in range(2):
        mask = half_mask(first[part].shape, half)
        out_ref[part] = jnp.where(mask, first[part], second[part])


def which(colour):
    return (colour + lax.axis_index("sa")) % 2


def fetch(pairs, sem):
    copies = [pltpu.make_async_copy(source, target, sem.at[k]) for k, (source, target) in enumerate(pairs)]
    for copy in copies:
        copy.start()
    return copies


def turn_of(colour, late):
    early = lax.axis_index("ta") % 2 == which(colour)
    return jnp.logical_not(early) if late else early


def pack_kernel(late, *refs):
    steps_in, rhs_in, links_in, clover_in, *refs = refs
    if late:
        refs = refs[7:]
    (m_ref, time_ref, m_other_ref, time_other_ref, own_ref, other_ref, steps_ref,
     raw_ref, rhs_ref, count_ref, sem) = refs
    half = which(0)

    @pl.when(turn_of(0, late))
    def _():
        dof = rhs_ref.shape[1]
        pieces = []
        for term in range(5):
            source = clover_in if term == 0 else links_in.at[term % 4]
            for part in range(2):
                for row in range(0, dof, dof // PIECES):
                    rows = pl.ds(row, dof // PIECES)
                    pieces.append((source.at[part, rows], raw_ref.at[term, part, rows]))
        copies = fetch(pieces + [(rhs_in, rhs_ref), (steps_in, count_ref)], sem)
        for term in range(5):
            for copy in copies[2 * PIECES * term:2 * PIECES * (term + 1)]:
                copy.wait()
            if term == 4:
                pack_matrix(raw_ref.at[term], 1, time_ref, time_other_ref)
            else:
                pack_matrix(raw_ref.at[term], half, m_ref.at[term], m_other_ref.at[term])
            if term == 1:
                copies[-2].wait()
                copies[-1].wait()
                for k in range(2):
                    steps_ref[k] = jnp.full(steps_ref.shape[1:], count_ref[0, 0, k].astype(F32))
                own_ref[...] = pack_field(rhs_ref, half)
                other_ref[...] = pack_field(rhs_ref, 1 - half)


def first_kernel(late, steps_ref, r_ref, m_ref, time_ref, *refs):
    if late:
        refs = refs[3:]
    e_ref, s_ref, mz_ref, mt_ref, w_ref, *work = refs
    _, rows_ref, spread_ref, back_ref, _ = work
    half = which(0)
    mine = turn_of(0, late)
    relax(r_ref[...], steps_ref[half], m_ref, s_ref, e_ref, w_ref, work, mine, 8)

    @pl.when(mine)
    def _():
        send(half, e_ref[...], w_ref, mt_ref, mz_ref, time_ref, rows_ref, spread_ref, back_ref)


def local_part(half, e, base, time_ref, r_ref, ab_ref, rows_ref, spread_ref, back_ref, part_ref):
    @pl.when(half == 0)
    def _():
        r_ref[...] = base() + backward_product(e, time_ref, rows_ref, spread_ref, back_ref)

    @pl.when(half != 0)
    def _():
        put_forward(e, swap(e), ab_ref, 0)
        r_ref[...] = base() + forward_sums([(time_ref, 0)], ab_ref, part_ref)


def local_kernel(colour, e_ref, s_ref, time_ref, *refs):
    half = which(colour)
    if len(refs) > 6:
        x_here, x_other, r_ref, sol_ref, *work = refs
        unpack_fields(half, x_here[...], x_other[...], sol_ref)
    else:
        r_ref, *work = refs
    local_part(half, e_ref[...], lambda: s_ref[...], time_ref, r_ref, *work)


def remote_part(half, r, mt, mz_up, mz_down, m_ref, time_ref, ab_ref, part_ref):
    depth = lanes(r.shape) % (r.shape[1] // 2) // PLANE
    reach = (LZ - 1) * PLANE
    top = depth == LZ - 1
    put_forward(jnp.where(top, turn(mz_up, reach), 0.0), jnp.where(top, turn(mz_up, reach + r.shape[1] // 2), 0.0), ab_ref, 0)
    ahead = jnp.where(half == 0, 0.0, mt)
    put_forward(ahead, swap(ahead), ab_ref, 1)
    total = r + jnp.where(depth == 0, turn(mz_down, -reach), 0.0) + jnp.where(half == 0, mt, 0.0)
    return total + forward_sums([(m_ref.at[1], 0), (time_ref, 1)], ab_ref, part_ref)


def sweep_kernel(colour, n_t_in, n_z, fresh, late, *refs):
    steps_ref, r_ref, *refs = refs
    arrived = refs
    refs = refs[n_t_in + n_z:]
    m_ref, time_ref, *refs = refs
    if not fresh:
        sol_ref, *refs = refs
    if late:
        refs = refs[4:]
    e_ref, s_ref, new_ref, mz_ref, mt_ref, w_ref, *work = refs
    ab_ref, rows_ref, spread_ref, back_ref, part_ref = work
    half = which(colour)
    mine = None if late is None else turn_of(colour, late)
    always = True if late is None else mine

    @pl.when(always)
    def _():
        mt, mz_up, mz_down, _ = arrivals(arrived, colour, n_t_in, n_z)
        s_ref[...] = remote_part(half, r_ref[...], mt, mz_up, mz_down, m_ref, time_ref, ab_ref, part_ref)

    relax(None, steps_ref[half], m_ref, s_ref, e_ref, w_ref, work, mine)

    @pl.when(always)
    def _():
        send(half, e_ref[...], w_ref, mt_ref, mz_ref, time_ref, rows_ref, spread_ref, back_ref)
        new_ref[...] = e_ref[...] if fresh else sol_ref[...] + e_ref[...]


def arrivals(refs, colour, n_t_in, n_z):
    mt = refs[0][...]
    if n_t_in == 2:
        mt = jnp.where(turn_of(1 - colour, False), refs[1][...], mt)
    up, down = refs[n_t_in], refs[n_t_in + n_z - 1]
    return mt, up[...], down[...], refs[n_t_in + n_z:]


def last_kernel(colour, n_t_in, n_z, r_ref, *refs):
    mt, mz_up, mz_down, refs = arrivals(refs, colour, n_t_in, n_z)
    m_ref, time_ref, s_ref, res_ref, ab_ref, part_ref = refs
    half = which(colour)
    residual = remote_part(half, r_ref[...], mt, mz_up, mz_down, m_ref, time_ref, ab_ref, part_ref)
    unpack_fields(half, residual, s_ref[...], res_ref)


def shards(rhs, links, clover, mr_steps):
    dof = rhs.shape[2]
    width = rhs.shape[-1]
    rhs_local = rhs.reshape(2, dof, width)
    links_local = links.reshape(4, 2, dof, dof, width)
    clover_local = clover.reshape(2, dof, dof, width)
    n_t = lax.axis_size("ta")
    n_s = lax.axis_size("sa")
    n_z = 1 if n_s == 2 else 2

    vector = jax.ShapeDtypeStruct((dof, width), F32)
    matrix = jax.ShapeDtypeStruct((dof // 2, 2 * dof, width), BF16)
    matrices = jax.ShapeDtypeStruct((4,) + matrix.shape, BF16)
    counts = jax.ShapeDtypeStruct((2, 8, width), F32)
    pair = jax.ShapeDtypeStruct((2, dof, width), F32)
    field = pltpu.VMEM((dof, width), F32)
    ab = pltpu.VMEM((4, 2, 2, 2 * dof, width), BF16)
    part = pltpu.VMEM((2, dof // 2, 16, width), F32)
    work = [
        ab,
        pltpu.VMEM((2, dof, width), F32),
        pltpu.VMEM((2, 2, dof // 2, 16, width), BF16),
        pltpu.VMEM((4, 2, 2 * dof, width), F32),
        part,
    ]
    raw = pltpu.VMEM((5, 2, dof, dof, width), links.dtype)
    rhs_buffer = pltpu.VMEM((2, dof, width), F32)
    params = pltpu.CompilerParams(vmem_limit_bytes=20 << 20)

    def call(kernel, ins, outs, scratch, specs=None, aliases={}):
        return pl.pallas_call(
            kernel,
            in_specs=specs or [VMEM] * len(ins),
            out_specs=[VMEM] * len(outs),
            out_shape=outs,
            scratch_shapes=scratch,
            compiler_params=params,
            input_output_aliases=aliases,
        )(*ins)

    def time_pairs(colour, late=None):
        pairs = []
        for t in range(n_t):
            for s in range(n_s):
                half = (colour + s) % 2
                if late is None or (t % 2 != half) == late:
                    goal = (t + 1) % n_t if half else (t - 1) % n_t
                    pairs.append((t * n_s + s, goal * n_s + s))
                elif late and n_s % 2 == 0 and n_t % 2 == 0:
                    pairs.append((t * n_s + s, t * n_s + (s + 1) % n_s))
        return pairs

    def along_time(mt, colour, late=None):
        return lax.ppermute(mt, ("ta", "sa"), time_pairs(colour, late))

    def along_z(mz):
        got = [lax.ppermute(mz, "sa", [(s, (s - 1) % n_s) for s in range(n_s)])]
        if n_z == 2:
            got.append(lax.ppermute(mz, "sa", [(s, (s + 1) % n_s) for s in range(n_s)]))
        return got

    args = [pltpu.with_memory_space_constraint(v, pltpu.HBM) for v in (mr_steps, rhs_local, links_local, clover_local)]
    outs = [matrices, matrix, matrices, matrix, vector, vector, counts]
    scratch = [raw, rhs_buffer, pltpu.SMEM(mr_steps.shape, mr_steps.dtype), pltpu.SemaphoreType.DMA((10 * PIECES + 2,))]
    packed = call(functools.partial(pack_kernel, False), args, outs, scratch, [HBM] * 4)
    m0, time1, m1, time0, own, r, steps = packed
    early = call(functools.partial(first_kernel, False), [steps, own, m0, time1], [vector] * 4, [field] + work)
    mt_a = along_time(early[-1], 0, False)
    m0, time1, m1, time0, own, r, steps = call(
        functools.partial(pack_kernel, True), [*args, *packed], outs, scratch,
        [HBM] * 4 + [VMEM] * 7, {4 + k: k for k in range(7)},
    )
    e, s0, mz, mt = call(
        functools.partial(first_kernel, True), [steps, own, m0, time1, *early[:-1]], [vector] * 4,
        [field] + work, None, {4 + k: k for k in range(3)},
    )
    got = [mt_a, along_time(mt, 0, True), *along_z(mz)]

    def neighbours(colour, e, base, fields=()):
        outs = [vector, pair] if fields else [vector]
        return call(functools.partial(local_kernel, colour), [e, base, time0, *fields], outs, work)

    (r,) = neighbours(0, e, r)
    blocks = [m0, m1]
    x = [e, None]
    kept = [s0, None]
    last = 2 * SWEEPS - 1
    for index in range(1, last + 1):
        colour = index % 2
        ins = [steps, r, *got, blocks[colour], time1]
        fresh = x[colour] is None
        if not fresh:
            ins.append(x[colour])
        kernel = functools.partial(sweep_kernel, colour, len(got) - n_z, n_z, fresh)
        outs = [vector] * 5
        if index == 1:
            early = call(functools.partial(kernel, False), ins, outs, [field] + work)
            mt_a = along_time(early[-1], colour, False)
            e, kept[colour], x[colour], mz, mt = call(
                functools.partial(kernel, True), [*ins, *early[:-1]], outs, [field] + work,
                None, {len(ins) + k: k for k in range(4)},
            )
            got = [mt_a, along_time(mt, colour, True), *along_z(mz)]
        else:
            e, kept[colour], x[colour], mz, mt = call(functools.partial(kernel, None), ins, outs, [field] + work)
            got = [along_time(mt, colour), *along_z(mz)]
        fields = (x[colour], x[1 - colour]) if index == last else ()
        r, *sol = neighbours(colour, e, kept[1 - colour], fields)
    colour = (last + 1) % 2
    ins = [r, *got, blocks[colour], time1, kept[1 - colour]]
    (res,) = call(functools.partial(last_kernel, colour, len(got) - n_z, n_z), ins, [pair], [ab, part])
    return sol[0].reshape(rhs.shape), res.reshape(rhs.shape)


def solution(mesh):
    field = P(None, None, None, "ta", "sa", None)
    placed = (field, P(None, None, None, None, "ta", "sa", None), field, P("ta", "sa", None))
    return jax.shard_map(shards, mesh=mesh, in_specs=placed, out_specs=(field, field), check_vma=False)
```

```python
import functools

import jax
import jax.numpy as jnp
from jax import lax
from jax.experimental import pallas as pl
from jax.experimental.pallas import tpu as pltpu
from jax.sharding import PartitionSpec as P


LZ = 4
LY = 4
LX = 4
MR_MAX = 3
SWEEPS = 2
PLANE = LY * LX
UNIT = 4
PIECES = 1

F32 = jnp.float32
BF16 = jnp.bfloat16
VMEM = pl.BlockSpec(memory_space=pltpu.VMEM)
HBM = pl.BlockSpec(memory_space=pltpu.HBM)


def lanes(shape):
    return lax.broadcasted_iota(jnp.int32, shape, len(shape) - 1)


def sublanes(shape):
    return lax.broadcasted_iota(jnp.int32, shape, len(shape) - 2)


def low_half(shape):
    return lanes(shape) < shape[-1] // 2


def real_rows(shape):
    return sublanes(shape) % (2 * UNIT) < UNIT


def turn(x, amount):
    amount %= x.shape[-1]
    return pltpu.roll(x, amount, x.ndim - 1) if amount else x


def swap(x):
    return turn(x, x.shape[-1] // 2)


def tiles(x):
    return [x[k:k + 2 * UNIT] for k in range(0, x.shape[0], 2 * UNIT)]


def flip(x):
    return jnp.concatenate([pltpu.roll(t, UNIT, 0) for t in tiles(x)], 0)


def times_i(x):
    return jnp.where(real_rows(x.shape), -1.0, 1.0) * flip(x)


def chirality(shape):
    return jnp.where(low_half(shape), 1.0, -1.0).astype(F32)


def shifted(x, direction, sign, extra):
    place = lanes(x.shape) % (x.shape[-1] // 2)
    extent, stride = {1: (LZ, PLANE), 2: (LY, LX), 3: (LX, 1)}[direction]
    edge = place // stride % extent == (extent - 1 if sign > 0 else 0)
    inner = turn(x, extra - sign * stride)
    if direction == 1:
        return jnp.where(edge, jnp.zeros_like(inner), inner)
    return jnp.where(edge, turn(x, extra + sign * (extent - 1) * stride), inner)


def natural(x, y):
    low = low_half((2 * UNIT, x.shape[1]))
    real = real_rows(low.shape)
    pairs = list(zip(tiles(x), tiles(y)))
    units = [jnp.where(low, a, b) for a, b in pairs] + [jnp.where(low, b, a) for a, b in pairs]
    re, im = [], []
    for even, odd in zip(units[0::2], units[1::2]):
        re.append(jnp.where(real, even, pltpu.roll(odd, UNIT, 0)))
        im.append(jnp.where(real, pltpu.roll(even, UNIT, 0), odd))
    return jnp.concatenate(re, 0), jnp.concatenate(im, 0)


def unit_tiles(re, im):
    real = real_rows((2 * UNIT, re.shape[1]))
    out = []
    for a, b in zip(tiles(re), tiles(im)):
        out.append(jnp.where(real, a, pltpu.roll(b, UNIT, 0)))
        out.append(jnp.where(real, pltpu.roll(a, UNIT, 0), b))
    return out


def split(x):
    high = x.astype(BF16).astype(F32)
    return high, x - high


def gather_rows(parts):
    rows = sublanes(parts[0].shape)
    step = 1
    while len(parts) > 1:
        upper = (rows & step) != 0
        parts = [
            jnp.where(upper, odd, even) + pltpu.roll(jnp.where(upper, even, odd), step, 0)
            for even, odd in zip(parts[0::2], parts[1::2])
        ]
        step *= 2
    return parts[0]


def put_forward(x, y, ab_ref, slot):
    re, im = natural(x, y)
    for k, (r, i) in enumerate(zip(split(re), split(im))):
        ab_ref[slot, 0, k] = jnp.concatenate([r, -i], 0).astype(BF16)
        ab_ref[slot, 1, k] = jnp.concatenate([i, r], 0).astype(BF16)


def put_backward(x, rows_ref, spread_ref):
    dof, width = x.shape
    for k, part in enumerate(split(x * chirality(x.shape))):
        rows_ref[k] = part
        for row in range(dof):
            r, kind = UNIT * (row // (2 * UNIT)) + row % UNIT, row // UNIT % 2
            spread_ref[kind, k, r] = jnp.broadcast_to(rows_ref[k, row:row + 1, :], (16, width)).astype(BF16)


def forward_sums(terms, ab_ref, part_ref, unroll=1, start=0):
    entries, rows, _ = terms[0][0].shape

    def body(group, carry):
        for own in range(2):
            r = 2 * group + own
            for kind in range(2):
                total = None
                for m_ref, slot in terms:
                    for t in range(0, rows, 16):
                        m = m_ref[r + start, pl.ds(t, 16), :].astype(F32)
                        for k in range(2):
                            product = m * ab_ref[slot, kind, k, pl.ds(t, 16), :].astype(F32)
                            total = product if total is None else total + product
                part_ref[kind, r] = total
        return carry

    lax.fori_loop(0, entries // 2, body, 0, unroll=unroll)
    out = []
    for t in range(0, entries, UNIT):
        parts = [part_ref[kind, t + k, 0:8, :] + part_ref[kind, t + k, 8:16, :] for kind in range(2) for k in range(UNIT)]
        out.append(gather_rows(parts))
    return jnp.concatenate(out, 0)


def backward_sums(m_ref, spread_ref, back_ref):
    entries, rows, _ = m_ref.shape
    for t in range(0, rows, 16):
        for kind in range(2):
            total = None
            for r in range(entries):
                m = m_ref[r, pl.ds(t, 16), :].astype(F32)
                for k in range(2):
                    product = m * spread_ref[kind, k, r].astype(F32)
                    total = product if total is None else total + product
            back_ref[kind, pl.ds(t, 16), :] = total


def backward_halves(back_ref):
    dof = back_ref.shape[1] // 2
    re = back_ref[0, 0:dof, :] + back_ref[1, dof:2 * dof, :]
    im = back_ref[1, 0:dof, :] - back_ref[0, dof:2 * dof, :]
    units = unit_tiles(re, im)
    half = len(units) // 2
    low = low_half(units[0].shape)
    a = [jnp.where(low, p, q) for p, q in zip(units[:half], units[half:])]
    b = [jnp.where(low, q, p) for p, q in zip(units[:half], units[half:])]
    return jnp.concatenate(a, 0), jnp.concatenate(b, 0)


def block_operator(x, unroll, start, m_ref, ab_ref, rows_ref, spread_ref, back_ref, part_ref):
    half = x.shape[1] // 2
    put_forward(x, swap(x), ab_ref, 0)
    for kind in range(2):
        for k in range(2):
            hopped = -ab_ref[0, kind, k]
            for direction in (1, 2, 3):
                ab_ref[direction, kind, k] = shifted(hopped, direction, 1, 0)
    put_backward(x, rows_ref, spread_ref)

    for direction in (1, 2, 3):
        backward_sums(m_ref.at[direction], spread_ref, back_ref.at[direction])
    total = forward_sums([(m_ref.at[term], term) for term in range(4)], ab_ref, part_ref, unroll, start)
    backs = 0.0
    for direction in (1, 2, 3):
        a, b = backward_halves(back_ref.at[direction])
        backs = backs + shifted(a, direction, -1, 0) + shifted(b, direction, -1, half)
        if direction == 1:
            back_z = chirality(x.shape) * (a + swap(b))
    return total - chirality(x.shape) * backs, back_z


def backward_product(x, m_ref, rows_ref, spread_ref, back_ref):
    put_backward(x, rows_ref, spread_ref)
    backward_sums(m_ref, spread_ref, back_ref.at[0])
    a, b = backward_halves(back_ref.at[0])
    return chirality(x.shape) * (a + swap(b))


def total_of(x):
    parts = tiles(x)
    total = parts[0]
    for part in parts[1:]:
        total = total + part
    for amount in (4, 2, 1):
        total = total + pltpu.roll(total, amount, 0)
    return jnp.broadcast_to(jnp.sum(total, axis=1, keepdims=True), total.shape)


def scaled(alpha, x):
    return jnp.concatenate([alpha * tile for tile in tiles(x)], 0)


def relax(residual, steps, m_ref, s_ref, e_ref, w_ref, work, mine=None, trips=4):
    @pl.when(True if mine is None else mine)
    def _():
        if residual is not None:
            s_ref[...] = residual
        e_ref[...] = jnp.zeros_like(e_ref)
        w_ref[...] = jnp.zeros_like(w_ref)

    def step(index, carry):
        s = s_ref[...]
        q, back_z = block_operator(s, s.shape[0] // trips, jnp.minimum(index, 0), m_ref, *work)
        s = s_ref[...]
        i_s = times_i(s)
        scale = total_of(q * q) + 1e-6
        alpha_re = total_of(q * s) / scale
        alpha_im = -total_of(q * i_s) / scale
        e_ref[...] += scaled(alpha_re, s) + scaled(alpha_im, i_s)
        w_ref[...] += scaled(alpha_re, back_z) + scaled(alpha_im, times_i(back_z))
        s_ref[...] = s - (scaled(alpha_re, q) + scaled(alpha_im, times_i(q)))
        return carry

    count = jnp.minimum(steps[0, 0], MR_MAX)
    lax.fori_loop(0, count if mine is None else jnp.where(mine, count, 0), step, 0)


def send(half, e, w_ref, mt_ref, mz_ref, time_ref, rows_ref, spread_ref, back_ref):
    place = lanes(e.shape) % (e.shape[-1] // 2)
    mz_ref[...] = jnp.where(place // PLANE == 0, e, w_ref[...])

    @pl.when(half == 0)
    def _():
        mt_ref[...] = e

    @pl.when(half != 0)
    def _():
        mt_ref[...] = backward_product(e, time_ref, rows_ref, spread_ref, back_ref)


def half_mask(shape, half):
    return low_half(shape) == (half == 0)


def pack_matrix(raw_ref, half, own_ref, other_ref):
    dof = raw_ref.shape[1]
    entries = dof // 2
    mask = half_mask((dof, raw_ref.shape[-1]), half)

    def body(r, carry):
        for part in range(2):
            near = raw_ref[part, r + entries * half].astype(F32)
            far = raw_ref[part, r + entries * (1 - half)].astype(F32)
            own_ref[r, pl.ds(part * dof, dof), :] = jnp.where(mask, near, swap(far)).astype(BF16)
            other_ref[r, pl.ds(part * dof, dof), :] = jnp.where(mask, swap(near), far).astype(BF16)
        return carry

    lax.fori_loop(0, entries, body, 0, unroll=10)


def pack_field(ref, half):
    units = unit_tiles(ref[0], ref[1])
    count = len(units) // 2
    mask = half_mask(units[0].shape, half)
    first = jnp.concatenate(units[:count], 0)
    second = jnp.concatenate(units[count:], 0)
    own = jnp.where(half == 0, first, second)
    other = jnp.where(half == 0, second, first)
    return jnp.where(half_mask(own.shape, half), own, swap(other))


def unpack_fields(half, here, other, out_ref):
    first = natural(here, swap(here))
    second = natural(other, swap(other))
    for part in range(2):
        mask = half_mask(first[part].shape, half)
        out_ref[part] = jnp.where(mask, first[part], second[part])


def which(colour):
    return (colour + lax.axis_index("sa")) % 2


def fetch(pairs, sem):
    copies = [pltpu.make_async_copy(source, target, sem.at[k]) for k, (source, target) in enumerate(pairs)]
    for copy in copies:
        copy.start()
    return copies


def turn_of(colour, late):
    early = lax.axis_index("ta") % 2 == which(colour)
    return jnp.logical_not(early) if late else early


def pack_kernel(late, *refs):
    steps_in, rhs_in, links_in, clover_in, *refs = refs
    if late:
        refs = refs[7:]
    (m_ref, time_ref, m_other_ref, time_other_ref, own_ref, other_ref, steps_ref,
     raw_ref, rhs_ref, count_ref, sem) = refs
    half = which(0)

    @pl.when(turn_of(0, late))
    def _():
        dof = rhs_ref.shape[1]
        pieces = []
        for term in range(5):
            source = clover_in if term == 0 else links_in.at[term % 4]
            for part in range(2):
                for row in range(0, dof, dof // PIECES):
                    rows = pl.ds(row, dof // PIECES)
                    pieces.append((source.at[part, rows], raw_ref.at[term, part, rows]))
        copies = fetch(pieces + [(rhs_in, rhs_ref), (steps_in, count_ref)], sem)
        for term in range(5):
            for copy in copies[2 * PIECES * term:2 * PIECES * (term + 1)]:
                copy.wait()
            if term == 4:
                pack_matrix(raw_ref.at[term], 1, time_ref, time_other_ref)
            else:
                pack_matrix(raw_ref.at[term], half, m_ref.at[term], m_other_ref.at[term])
            if term == 1:
                copies[-2].wait()
                copies[-1].wait()
                for k in range(2):
                    steps_ref[k] = jnp.full(steps_ref.shape[1:], count_ref[0, 0, k])
                own_ref[...] = pack_field(rhs_ref, half)
                other_ref[...] = pack_field(rhs_ref, 1 - half)


def first_kernel(late, steps_ref, r_ref, m_ref, time_ref, *refs):
    if late:
        refs = refs[3:]
    e_ref, s_ref, mz_ref, mt_ref, w_ref, *work = refs
    _, rows_ref, spread_ref, back_ref, _ = work
    half = which(0)
    mine = turn_of(0, late)
    relax(r_ref[...], steps_ref[half], m_ref, s_ref, e_ref, w_ref, work, mine, 8)

    @pl.when(mine)
    def _():
        send(half, e_ref[...], w_ref, mt_ref, mz_ref, time_ref, rows_ref, spread_ref, back_ref)


def local_part(half, e, base, time_ref, r_ref, ab_ref, rows_ref, spread_ref, back_ref, part_ref):
    @pl.when(half == 0)
    def _():
        r_ref[...] = base() + backward_product(e, time_ref, rows_ref, spread_ref, back_ref)

    @pl.when(half != 0)
    def _():
        put_forward(e, swap(e), ab_ref, 0)
        r_ref[...] = base() + forward_sums([(time_ref, 0)], ab_ref, part_ref)


def local_kernel(colour, e_ref, s_ref, time_ref, *refs):
    half = which(colour)
    if len(refs) > 6:
        x_here, x_other, r_ref, sol_ref, *work = refs
        unpack_fields(half, x_here[...], x_other[...], sol_ref)
    else:
        r_ref, *work = refs
    local_part(half, e_ref[...], lambda: s_ref[...], time_ref, r_ref, *work)


def remote_part(half, r, mt, mz_up, mz_down, m_ref, time_ref, ab_ref, part_ref):
    depth = lanes(r.shape) % (r.shape[1] // 2) // PLANE
    reach = (LZ - 1) * PLANE
    top = depth == LZ - 1
    put_forward(jnp.where(top, turn(mz_up, reach), 0.0), jnp.where(top, turn(mz_up, reach + r.shape[1] // 2), 0.0), ab_ref, 0)
    ahead = jnp.where(half == 0, 0.0, mt)
    put_forward(ahead, swap(ahead), ab_ref, 1)
    total = r + jnp.where(depth == 0, turn(mz_down, -reach), 0.0) + jnp.where(half == 0, mt, 0.0)
    return total + forward_sums([(m_ref.at[1], 0), (time_ref, 1)], ab_ref, part_ref)


def sweep_kernel(colour, n_t_in, n_z, fresh, late, *refs):
    steps_ref, r_ref, *refs = refs
    arrived = refs
    refs = refs[n_t_in + n_z:]
    m_ref, time_ref, *refs = refs
    if not fresh:
        sol_ref, *refs = refs
    if late:
        refs = refs[4:]
    e_ref, s_ref, new_ref, mz_ref, mt_ref, w_ref, *work = refs
    ab_ref, rows_ref, spread_ref, back_ref, part_ref = work
    half = which(colour)
    mine = None if late is None else turn_of(colour, late)
    always = True if late is None else mine

    @pl.when(always)
    def _():
        mt, mz_up, mz_down, _ = arrivals(arrived, colour, n_t_in, n_z)
        s_ref[...] = remote_part(half, r_ref[...], mt, mz_up, mz_down, m_ref, time_ref, ab_ref, part_ref)

    relax(None, steps_ref[half], m_ref, s_ref, e_ref, w_ref, work, mine)

    @pl.when(always)
    def _():
        send(half, e_ref[...], w_ref, mt_ref, mz_ref, time_ref, rows_ref, spread_ref, back_ref)
        new_ref[...] = e_ref[...] if fresh else sol_ref[...] + e_ref[...]


def arrivals(refs, colour, n_t_in, n_z):
    mt = refs[0][...]
    if n_t_in == 2:
        mt = jnp.where(turn_of(1 - colour, False), refs[1][...], mt)
    up, down = refs[n_t_in], refs[n_t_in + n_z - 1]
    return mt, up[...], down[...], refs[n_t_in + n_z:]


def last_kernel(colour, n_t_in, n_z, r_ref, *refs):
    mt, mz_up, mz_down, refs = arrivals(refs, colour, n_t_in, n_z)
    m_ref, time_ref, s_ref, res_ref, ab_ref, part_ref = refs
    half = which(colour)
    residual = remote_part(half, r_ref[...], mt, mz_up, mz_down, m_ref, time_ref, ab_ref, part_ref)
    unpack_fields(half, residual, s_ref[...], res_ref)


def shards(rhs, links, clover, mr_steps):
    dof = rhs.shape[2]
    width = rhs.shape[-1]
    rhs_local = rhs.reshape(2, dof, width)
    links_local = links.reshape(4, 2, dof, dof, width)
    clover_local = clover.reshape(2, dof, dof, width)
    n_t = lax.axis_size("ta")
    n_s = lax.axis_size("sa")
    n_z = 1 if n_s == 2 else 2

    vector = jax.ShapeDtypeStruct((dof, width), F32)
    matrix = jax.ShapeDtypeStruct((dof // 2, 2 * dof, width), BF16)
    matrices = jax.ShapeDtypeStruct((4,) + matrix.shape, BF16)
    counts = jax.ShapeDtypeStruct((2, 8, width), jnp.int32)
    pair = jax.ShapeDtypeStruct((2, dof, width), F32)
    field = pltpu.VMEM((dof, width), F32)
    ab = pltpu.VMEM((4, 2, 2, 2 * dof, width), BF16)
    part = pltpu.VMEM((2, dof // 2, 16, width), F32)
    work = [
        ab,
        pltpu.VMEM((2, dof, width), F32),
        pltpu.VMEM((2, 2, dof // 2, 16, width), BF16),
        pltpu.VMEM((4, 2, 2 * dof, width), F32),
        part,
    ]
    raw = pltpu.VMEM((5, 2, dof, dof, width), links.dtype)
    rhs_buffer = pltpu.VMEM((2, dof, width), F32)
    params = pltpu.CompilerParams(vmem_limit_bytes=20 << 20)

    def call(kernel, ins, outs, scratch, specs=None, aliases={}):
        return pl.pallas_call(
            kernel,
            in_specs=specs or [VMEM] * len(ins),
            out_specs=[VMEM] * len(outs),
            out_shape=outs,
            scratch_shapes=scratch,
            compiler_params=params,
            input_output_aliases=aliases,
        )(*ins)

    def time_pairs(colour, late=None):
        pairs = []
        for t in range(n_t):
            for s in range(n_s):
                half = (colour + s) % 2
                if late is None or (t % 2 != half) == late:
                    goal = (t + 1) % n_t if half else (t - 1) % n_t
                    pairs.append((t * n_s + s, goal * n_s + s))
                elif late and n_s % 2 == 0 and n_t % 2 == 0:
                    pairs.append((t * n_s + s, t * n_s + (s + 1) % n_s))
        return pairs

    def along_time(mt, colour, late=None):
        return lax.ppermute(mt, ("ta", "sa"), time_pairs(colour, late))

    def along_z(mz):
        got = [lax.ppermute(mz, "sa", [(s, (s - 1) % n_s) for s in range(n_s)])]
        if n_z == 2:
            got.append(lax.ppermute(mz, "sa", [(s, (s + 1) % n_s) for s in range(n_s)]))
        return got

    args = [pltpu.with_memory_space_constraint(v, pltpu.HBM) for v in (mr_steps, rhs_local, links_local, clover_local)]
    outs = [matrices, matrix, matrices, matrix, vector, vector, counts]
    scratch = [raw, rhs_buffer, pltpu.SMEM(mr_steps.shape, mr_steps.dtype), pltpu.SemaphoreType.DMA((10 * PIECES + 2,))]
    packed = call(functools.partial(pack_kernel, False), args, outs, scratch, [HBM] * 4)
    m0, time1, m1, time0, own, r, steps = packed
    early = call(functools.partial(first_kernel, False), [steps, own, m0, time1], [vector] * 4, [field] + work)
    mt_a = along_time(early[-1], 0, False)
    m0, time1, m1, time0, own, r, steps = call(
        functools.partial(pack_kernel, True), [*args, *packed], outs, scratch,
        [HBM] * 4 + [VMEM] * 7, {4 + k: k for k in range(7)},
    )
    e, s0, mz, mt = call(
        functools.partial(first_kernel, True), [steps, own, m0, time1, *early[:-1]], [vector] * 4,
        [field] + work, None, {4 + k: k for k in range(3)},
    )
    got = [mt_a, along_time(mt, 0, True), *along_z(mz)]

    def neighbours(colour, e, base, fields=()):
        outs = [vector, pair] if fields else [vector]
        return call(functools.partial(local_kernel, colour), [e, base, time0, *fields], outs, work)

    (r,) = neighbours(0, e, r)
    blocks = [m0, m1]
    x = [e, None]
    kept = [s0, None]
    last = 2 * SWEEPS - 1
    for index in range(1, last + 1):
        colour = index % 2
        ins = [steps, r, *got, blocks[colour], time1]
        fresh = x[colour] is None
        if not fresh:
            ins.append(x[colour])
        kernel = functools.partial(sweep_kernel, colour, len(got) - n_z, n_z, fresh)
        outs = [vector] * 5
        if index == 1:
            early = call(functools.partial(kernel, False), ins, outs, [field] + work)
            mt_a = along_time(early[-1], colour, False)
            e, kept[colour], x[colour], mz, mt = call(
                functools.partial(kernel, True), [*ins, *early[:-1]], outs, [field] + work,
                None, {len(ins) + k: k for k in range(4)},
            )
            got = [mt_a, along_time(mt, colour, True), *along_z(mz)]
        else:
            e, kept[colour], x[colour], mz, mt = call(functools.partial(kernel, None), ins, outs, [field] + work)
            got = [along_time(mt, colour), *along_z(mz)]
        fields = (x[colour], x[1 - colour]) if index == last else ()
        r, *sol = neighbours(colour, e, kept[1 - colour], fields)
    colour = (last + 1) % 2
    ins = [r, *got, blocks[colour], time1, kept[1 - colour]]
    (res,) = call(functools.partial(last_kernel, colour, len(got) - n_z, n_z), ins, [pair], [ab, part])
    return sol[0].reshape(rhs.shape), res.reshape(rhs.shape)


def solution(mesh):
    field = P(None, None, None, "ta", "sa", None)
    placed = (field, P(None, None, None, None, "ta", "sa", None), field, P("ta", "sa", None))
    return jax.shard_map(shards, mesh=mesh, in_specs=placed, out_specs=(field, field), check_vma=False)
```
